32 devices in a mesh: grp: 2 (over y), row: 4 (over x, core), col: 4 (over z).
Axes of the slice: x: 2, y: 2, z: 4, core: 2. Of those that a mesh axis runs over, the one named last changes fastest.
Arguments:
- sigma_anc: float32 [1536, 768], P(('grp', 'row'), 'col'), parts along dimension 0, may hold values from -3 to 23, as said below
- anc_factor: float32 [1536, 2, 512], P(('grp', 'row', 'col')), parts along dimension 0, may hold values from -0.625 to 0.625
- diag_inverse: float32 [4, 512, 512], P('grp', None, 'row'), parts along dimension 0, may hold values from -0.6 to 1.5, as said below
- pattern: int32 [2, 6], replicated, may hold values from 0 to 1, as said below
Outputs:
- sel_off: float32 [1536, 2, 512], P(('grp', 'row', 'col')), parts along dimension 0
- sel_diag: float32 [4, 512, 512], P('grp'), parts along dimension 0
The draws below stay inside these ranges and needn't reach their ends.
There are 2 independent parts, one for each index of `grp`. The reference program is written for one: setup_inputs(seed, part) draws one part's arguments, and reference() takes and returns one part's arrays. A program takes and returns all parts, laid end to end along the dimension named above; an argument that names none is the same for every part. Nothing has to cross between parts.
Inputs may be any that keep to these rules, and one draw needn't show every extreme that they name: `pattern`: each supernode's present row blocks are a run of consecutive blocks, wrapping around the end, of at least 0 blocks, at most 3, together with some scattered others. `sigma_anc`: symmetric and positive definite. `diag_inverse`: lower triangular, with diagonal entries between 0.5 and 1.5 and small entries below the diagonal.
All inputs are finite; a program needn't handle non-finite values.
Results may differ from the reference program's by a relative error of at most 0.00013.
Values sent between devices are 32-bit elements; how exact they have to be, the bound alone decides.
A program may use at most 64 MiB of HBM per device.

```python
import math
import jax
import jax.numpy as jnp
from jax import lax

WID = 512
SUPERS = 2
BLK = 128
R = 768
NBLK = 6


def draw_sigma_anc(key, part):
    key = jax.random.fold_in(key, 11)
    key_noise, key_diag = jax.random.split(key, 2)
    noise = jax.random.normal(key_noise, (R, R), jnp.float32)
    matrix = (noise + jnp.transpose(noise)) * (0.3 / math.sqrt(R))
    diagonal = jax.random.uniform(key_diag, (R,), jnp.float32, 1.0, 2.0)
    matrix = matrix + jnp.diag(diagonal)
    return matrix


def draw_diag_inverse(key, part):
    key = jax.random.fold_in(key, 23)
    key_noise, key_diag = jax.random.split(key, 2)
    noise = jax.random.normal(key_noise, (SUPERS, WID, WID), jnp.float32) * (0.5 / math.sqrt(WID))
    lower = jnp.tril(noise, -1)
    diagonal = jax.random.uniform(key_diag, (SUPERS, WID), jnp.float32, 0.5, 1.5)
    identity = jnp.eye(WID, dtype=jnp.float32)
    return lower + diagonal[:, :, None] * identity[None, :, :]


def draw_pattern(key, part):
    key = jax.random.fold_in(key, 37)
    key_start, key_length, key_extra = jax.random.split(key, 3)
    first_block = jax.random.randint(key_start, (SUPERS, 1), 0, NBLK)
    run_length = jax.random.randint(key_length, (SUPERS, 1), max(1, NBLK // 8), NBLK // 2 + 1)
    positions = jnp.arange(NBLK, dtype=jnp.int32)[None, :]
    inside = (positions - first_block) % NBLK < run_length
    scattered = jax.random.randint(key_extra, (SUPERS, NBLK), 0, 8) == 0
    return jnp.where(inside | scattered, 1, 0).astype(jnp.int32)


def levels(stream_key, shape, cuts, smallest, top_value):
    gain = 1.0
    for position, blocks in cuts:
        heights = jax.random.uniform(jax.random.fold_in(jax.random.fold_in(stream_key, 6), position), (blocks,), jnp.float32, smallest / len(cuts), top_value / len(cuts))
        gain = gain * jnp.repeat(jnp.exp(heights), shape[position] // blocks).reshape((-1,) + (1,) * (len(shape) - 1 - position))
    return gain


def scatter_about(own_key, shape, width, bound, cuts=(), held_as=jnp.bfloat16):
    result = jax.random.normal(own_key, shape, jnp.float32) * width
    if len(cuts) > 0:
        result = levels(own_key, shape, cuts, -0.22, 0.18) * result
    return jnp.clip(result, min=-bound, max=bound).astype(held_as)


def setup_inputs(seed: int = 0, part: int = 0) -> dict:
    keys = jax.random.split(jax.random.key(seed), 5)
    part_keys = jax.random.split(jax.random.fold_in(keys[4], part), 5)
    return {
        "sigma_anc": draw_sigma_anc(jax.random.fold_in(jax.random.fold_in(keys[4], part), 71), part),
        "anc_factor": scatter_about(part_keys[1], (R, SUPERS, WID), (R // 8) ** -0.5, 0.625, ((0, 16),), jnp.float32),
        "diag_inverse": draw_diag_inverse(jax.random.fold_in(jax.random.fold_in(keys[4], part), 71), part),
        "pattern": draw_pattern(jax.random.fold_in(keys[4], 71), part),
    }


def reference(sigma_anc, anc_factor, diag_inverse, pattern):
    precise = lax.Precision.HIGHEST
    row_mask = jnp.repeat(pattern.astype(jnp.float32), BLK, axis=1)
    mask_rows = jnp.transpose(row_mask)[:, :, None]
    scaled = jnp.einsum("rsk,skj->rsj", anc_factor, diag_inverse, precision=precise) * mask_rows
    flattened = scaled.reshape(R, SUPERS * WID)
    product = jnp.dot(sigma_anc, flattened, precision=precise, preferred_element_type=jnp.float32)
    sel_off = -(product.reshape(R, SUPERS, WID) * mask_rows)
    first_term = jnp.einsum("skj,skl->sjl", diag_inverse, diag_inverse, precision=precise)
    second_term = jnp.einsum("rsj,rsl->sjl", scaled, sel_off, precision=precise)
    sel_diag = first_term - second_term
    return sel_off, sel_diag
```

```python
import functools

import jax
import jax.numpy as jnp
from jax import lax
from jax.experimental import pallas as pl
from jax.experimental.pallas import tpu as pltpu
from jax.sharding import PartitionSpec as P

LANES = 128
SUBLANES = 8


def split(x):
    high = x.astype(jnp.bfloat16)
    low = (x - high.astype(jnp.float32)).astype(jnp.bfloat16)
    return high, low


def dot3(a, b, contract=((1,), (0,))):
    (ah, al), (bh, bl) = a, b
    f = lambda u, v: lax.dot_general(u, v, (contract, ((), ())), preferred_element_type=jnp.float32)
    return f(ah, bh) + (f(ah, bl) + f(al, bh))


def fused_kernel(
    n_r, n_c, supers, width, rows_dev, block_size,
    sig_ref, a_ref, d_ref, pat_ref,
    off_ref, res,
    av, ag, sig_t, sq, dfull, pbuf, rbuf, sbuf, rbuf2, left, right, goth, gown, grecv, hx, hrecv, zs, zrecv,
    send_sems, s_ag, s_sq, s_d, s_p, s_p2, s_g, s_h, s_z, s_zag, s_xag, s_sib, local_sems,
):
    r = lax.axis_index("row")
    c = lax.axis_index("col")
    n_x = n_r // 2
    x = r // 2
    k = r % 2
    sib = 2 * x + 1 - k
    piece = width // n_r
    nb = width // LANES
    half_rows = nb * (nb + 1) // 2 * LANES
    q = half_rows // (n_x * n_c)
    share = width // (n_r * n_c)
    block_rows = rows_dev * n_c
    sends = []

    def rcopy(src, dst, rsem, row, col):
        cp = pltpu.make_async_remote_copy(
            src_ref=src, dst_ref=dst, send_sem=send_sems.at[len(sends)], recv_sem=rsem,
            device_id={"row": row, "col": col}, device_id_type=pl.DeviceIdType.MESH,
        )
        cp.start()
        sends.append(cp)

    def wait_recv(dst, rsem):
        pltpu.make_async_copy(dst, dst, rsem).wait()

    barrier = pltpu.get_barrier_semaphore()
    sig = lambda row, col: pl.semaphore_signal(
        barrier, inc=1, device_id={"row": row, "col": col}, device_id_type=pl.DeviceIdType.MESH
    )
    for dc in range(1, n_c):
        sig(r, (c + dc) % n_c)
    sig(sib, c)
    for dx in range(1, n_x):
        sig(2 * ((x + dx) % n_x) + k, c)

    pl.semaphore_wait(barrier, n_c + n_x - 1)

    for h in range(supers):
        for t in range(nb):
            rows = a_ref[pl.ds(t * supers + h, rows_dev, stride=nb * supers), :]
            av[:, h * width + t * LANES : h * width + (t + 1) * LANES] = rows

    n_line = 70
    part_of = lambda j, h: ag.at[j, :, pl.ds(h * width, width)]
    own_part = lambda h: av.at[:, pl.ds(h * width, width)]

    def line_copy(src, j, d, to, h):
        slot = n_line + (2 * d + (1 if to > 0 else 0)) * supers + h
        return pltpu.make_async_remote_copy(
            src_ref=src, dst_ref=part_of(j, h), send_sem=send_sems.at[slot], recv_sem=s_ag.at[j * supers + h],
            device_id={"row": r, "col": (c + to + n_c) % n_c}, device_id_type=pl.DeviceIdType.MESH,
        )

    def line(d, to, f):
        for cc in range(n_c):
            j = cc - to * d
            if 0 <= j < n_c:
                @pl.when(c == cc)
                def _():
                    f(j, 0 <= cc + to < n_c)

    def start_own(j, onward, to, h):
        if onward:
            line_copy(own_part(h), j, 0, to, h).start()

    for h in range(supers):
        for to in (1, -1):
            line(0, to, functools.partial(start_own, to=to, h=h))
    d_slice = lambda ref, rr: ref.at[:, pl.ds(rr * piece, width - rr * piece), pl.ds(rr * piece, piece)]
    d_src = lambda rr: d_ref.at[:, pl.ds(rr * piece, width - rr * piece), :]

    def d_copy(src, rr, slot, row):
        return pltpu.make_async_remote_copy(
            src_ref=src, dst_ref=d_slice(dfull, rr), send_sem=send_sems.at[slot], recv_sem=s_d.at[rr],
            device_id={"row": row, "col": c}, device_id_type=pl.DeviceIdType.MESH,
        )

    n_fixed = 64
    for rr in range(n_r):
        @pl.when(r == rr)
        def _():
            for dx in range(1, n_x):
                d_copy(d_src(rr), rr, n_fixed + dx, 2 * ((x + dx) % n_x) + k).start()
            d_copy(d_src(rr), rr, n_fixed, sib).start()
            pltpu.make_async_copy(d_src(rr), d_slice(dfull, rr), local_sems.at[0]).start()
    own_copy = pltpu.make_async_copy(av, ag.at[c], local_sems.at[1])
    own_copy.start()

    sig_t[...] = jnp.transpose(sig_ref[...])
    sig_rows = lambda j: pl.ds(pl.multiple_of(j * rows_dev, SUBLANES), rows_dev)
    for dc in range(1, n_c):
        j = (c + dc) % n_c
        rcopy(sig_t.at[sig_rows(j), :], sq.at[c], s_sq.at[c], r, j)
    sq[c] = sig_t[sig_rows(c), :]

    for rr in range(1, n_r):
        dfull[:, 0 : rr * piece, rr * piece : (rr + 1) * piece] = jnp.zeros((supers, rr * piece, piece), jnp.float32)

    def mask_of(first, rows, s):
        row = first + lax.broadcasted_iota(jnp.int32, (rows, 1), 0)
        m = jnp.zeros((rows, 1), jnp.float32)
        for b in range(pat_ref.shape[1]):
            inside = (row >= b * block_size) & (row < (b + 1) * block_size)
            m = jnp.where(inside, pat_ref[s, b].astype(jnp.float32), m)
        return m

    def pass_line(j, onward, to, d, h):
        wait_recv(part_of(j, h), s_ag.at[j * supers + h])
        if onward:
            line_copy(part_of(j, h), j, d, to, h).start()

    for d in range(1, n_c):
        for h in range(supers):
            for to in (1, -1):
                line(d, to, functools.partial(pass_line, to=to, d=d, h=h))

    for rr in range(n_r):
        @pl.when((rr % 2 == k) & (rr // 2 != x))
        def _():
            wait_recv(d_slice(dfull, rr), s_d.at[rr])
            d_copy(d_slice(dfull, rr), rr, n_fixed + n_x + rr // 2, sib).start()

    own_copy.wait()
    for dc in range(1, n_c):
        j = (c + dc) % n_c
        wait_recv(sq.at[j], s_sq.at[j])
    sigma_rows = split(sq[...].reshape(n_r * rows_dev, block_rows))

    for s in range(supers):
        cols = slice(s * width, (s + 1) * width)
        block = ag[:, :, cols].reshape(block_rows, width) * mask_of(r * block_rows, block_rows, s)
        part = dot3(sigma_rows, split(block))
        pbuf[:, :, cols] = part.reshape(n_r, rows_dev, width)
    for i in range(n_x):
        xo = (x + 1 + i) % n_x
        rcopy(pbuf.at[2 * xo + 1 - k], rbuf.at[xo], s_p.at[xo], sib, c)

    for rr in range(n_r):
        @pl.when((rr % 2 != k))
        def _():
            wait_recv(d_slice(dfull, rr), s_d.at[rr])

        @pl.when(r == rr)
        def _():
            pltpu.make_async_copy(d_src(rr), d_slice(dfull, rr), local_sems.at[0]).wait()

    for i in range(n_x):
        xo = (x + 1 + i) % n_x
        wait_recv(rbuf.at[xo], s_p.at[xo])
        sbuf[xo] = pbuf[2 * xo + k] + rbuf[xo]
        if i < n_x - 1:
            rcopy(sbuf.at[xo], rbuf2.at[x], s_p2.at[x], 2 * xo + k, c)

    t_first = (r * n_c + c) * rows_dev
    own_first = (r * n_c + c) * share
    masks = [mask_of(t_first, rows_dev, s) for s in range(supers)]
    step = 2 * LANES

    def times_d(rows_value, s, store):
        for j in range(0, width, step):
            xs = split(rows_value[:, j:])
            ds = split(dfull[s, j:, j : j + step])
            store(j, dot3(xs, ds))

    for s in range(supers):
        def store_scaled(j, v):
            left[s, 0:rows_dev, j : j + step] = -v
        times_d(av[:, s * width : (s + 1) * width] * masks[s], s, store_scaled)
        own = dfull[s, pl.ds(pl.multiple_of(own_first, SUBLANES), share), :]
        left[s, rows_dev:, :] = own
        right[s, rows_dev:, :] = own

    for dx in range(1, n_x):
        xo = (x + dx) % n_x
        wait_recv(rbuf2.at[xo], s_p2.at[xo])
    for s in range(supers):
        cols = slice(s * width, (s + 1) * width)
        y = sbuf[x, :, cols]
        for dx in range(1, n_x):
            y = y + rbuf2[(x + dx) % n_x, :, cols]
        def store_off(j, v):
            right[s, 0:rows_dev, j : j + step] = v
            for t in range(j // LANES, (j + step) // LANES):
                at = pl.ds(t * supers + s, rows_dev, stride=nb * supers)
                off_ref[at, :] = v[:, t * LANES - j : (t + 1) * LANES - j]
        times_d(y * (-masks[s]), s, store_off)

    def diag_part(s, dst):
        lh, ll = split(left[s])
        rh, rl = split(right[s])
        b = 0
        for i in range(nb):
            li = slice(i * LANES, (i + 1) * LANES)
            v = dot3((lh[:, li], ll[:, li]), (rh[:, : (i + 1) * LANES], rl[:, : (i + 1) * LANES]), ((0,), (0,)))
            for j in range(i + 1):
                dst[b * LANES : (b + 1) * LANES, :] = v[:, j * LANES : (j + 1) * LANES]
                b += 1

    diag_part(1 - k, goth)
    rcopy(goth, grecv, s_g.at[0], sib, c)

    diag_part(k, gown)
    wait_recv(grecv, s_g.at[0])

    rows_at = lambda xo, j: pl.ds(pl.multiple_of((xo * n_c + j) * q, SUBLANES), q)
    for i in range(n_c):
        j = (c + 1 + i) % n_c
        for dx in range(1, n_x):
            xo = (x + dx) % n_x
            at = rows_at(xo, j)
            hx[at, :] = gown[at, :] + grecv[at, :]
            rcopy(hx.at[at, :], hrecv.at[x, j], s_h.at[x * n_c + j], 2 * xo + k, c)
    for i in range(n_c):
        j = (c + 1 + i) % n_c
        at = rows_at(x, j)
        v = gown[at, :] + grecv[at, :]
        for dx in range(1, n_x):
            xo = (x + dx) % n_x
            wait_recv(hrecv.at[xo, j], s_h.at[xo * n_c + j])
            v = v + hrecv[xo, j]
        zs[j] = v
        if i < n_c - 1:
            rcopy(zs.at[j], zrecv.at[c], s_z.at[c], r, j)

    total = zs[c]
    for dc in range(1, n_c):
        j = (c + dc) % n_c
        wait_recv(zrecv.at[j], s_z.at[j])
        total = total + zrecv[j]
    mine = res.at[k, rows_at(x, c), :]
    res[k, rows_at(x, c), :] = total

    for dc in range(1, n_c):
        rcopy(mine, mine, s_zag.at[c], r, (c + dc) % n_c)
    def pass_on(j):
        chunk = res.at[k, rows_at(x, j), :]
        for dx in range(1, n_x):
            rcopy(chunk, chunk, s_xag.at[x * n_c + j], 2 * ((x + dx) % n_x) + k, c)
        rcopy(chunk, chunk, s_sib.at[x * n_c + j], sib, c)
    pass_on(c)
    for dc in range(1, n_c):
        j = (c + dc) % n_c
        wait_recv(res.at[k, rows_at(x, j), :], s_zag.at[j])
        pass_on(j)
    for dc in range(n_c):
        j = (c + dc) % n_c
        for dx in range(1, n_x):
            xo = (x + dx) % n_x
            chunk = res.at[k, rows_at(xo, j), :]
            wait_recv(chunk, s_xag.at[xo * n_c + j])
            rcopy(chunk, chunk, s_sib.at[xo * n_c + j], sib, c)

    for xo in range(n_x):
        for j in range(n_c):
            wait_recv(res.at[1 - k, rows_at(xo, j), :], s_sib.at[xo * n_c + j])

    for cp in sends:
        cp.wait_send()
    for rr in range(n_r):
        @pl.when(r == rr)
        def _():
            for dx in range(1, n_x):
                d_copy(d_src(rr), rr, n_fixed + dx, 2 * ((x + dx) % n_x) + k).wait_send()
            d_copy(d_src(rr), rr, n_fixed, sib).wait_send()

        @pl.when((rr % 2 == k) & (rr // 2 != x))
        def _():
            d_copy(d_slice(dfull, rr), rr, n_fixed + n_x + rr // 2, sib).wait_send()

    def sent(j, onward, to, d, h):
        if onward:
            line_copy(own_part(h), j, d, to, h).wait_send()

    for d in range(n_c):
        for h in range(supers):
            for to in (1, -1):
                line(d, to, functools.partial(sent, to=to, d=d, h=h))


def unpack_kernel(supers, nb, off_in, res, off_out, diag_out, stage, sems):
    copies = [pltpu.make_async_copy(off_in, off_out, sems.at[supers * nb])]
    copies[0].start()
    for s in range(supers):
        for i in range(nb):
            for j in range(nb):
                hi, lo = max(i, j), min(i, j)
                b = hi * (hi + 1) // 2 + lo
                v = res[s, b * LANES : (b + 1) * LANES, :]
                stage[s, i * LANES : (i + 1) * LANES, j * LANES : (j + 1) * LANES] = v if i >= j else jnp.transpose(v)
            at = (s, pl.ds(i * LANES, LANES))
            copies.append(pltpu.make_async_copy(stage.at[at], diag_out.at[at], sems.at[s * nb + i]))
            copies[-1].start()
    for cp in copies:
        cp.wait()


def fused_body(sigma_anc, anc_factor, diag_inverse, pattern):
    rows_dev, supers, width = anc_factor.shape
    n_r = lax.axis_size("row")
    n_c = lax.axis_size("col")
    n_x = n_r // 2
    total_rows = rows_dev * n_r * n_c
    flat = supers * width
    nb = width // LANES
    half_rows = nb * (nb + 1) // 2 * LANES
    q = half_rows // (n_x * n_c)
    share = width // (n_r * n_c)
    f32 = lambda *shape: pltpu.VMEM(shape, jnp.float32)
    dma = lambda n: pltpu.SemaphoreType.DMA((n,))
    vm = pl.BlockSpec(memory_space=pltpu.VMEM)
    linear = jnp.transpose(anc_factor.reshape(rows_dev, supers, nb, LANES), (0, 2, 1, 3))
    linear = linear.reshape(rows_dev * nb * supers, LANES)
    off, res = pl.pallas_call(
        functools.partial(fused_kernel, n_r, n_c, supers, width, rows_dev, total_rows // pattern.shape[1]),
        out_shape=(
            pltpu.VMEM((rows_dev * supers * nb, LANES), jnp.float32),
            pltpu.VMEM((supers, half_rows, LANES), jnp.float32),
        ),
        in_specs=[vm, vm, vm, pl.BlockSpec(memory_space=pltpu.SMEM)],
        out_specs=(vm, vm),
        scratch_shapes=[
            f32(rows_dev, flat),
            f32(n_c, rows_dev, flat),
            f32(n_r * rows_dev, n_c * rows_dev),
            f32(n_c, rows_dev, n_c * rows_dev),
            f32(supers, width, width),
            f32(n_r, rows_dev, flat),
            f32(n_x, rows_dev, flat),
            f32(n_x, rows_dev, flat),
            f32(n_x, rows_dev, flat),
            f32(supers, rows_dev + share, width),
            f32(supers, rows_dev + share, width),
            f32(half_rows, LANES),
            f32(half_rows, LANES),
            f32(half_rows, LANES),
            f32(half_rows, LANES),
            f32(n_x, n_c, q, LANES),
            f32(n_c, q, LANES),
            f32(n_c, q, LANES),
            dma(70 + 2 * n_c * supers),
            dma(n_c * supers), dma(n_c), dma(n_r), dma(n_x), dma(n_x), dma(1), dma(n_x * n_c), dma(n_c), dma(n_c),
            dma(n_x * n_c), dma(n_x * n_c), dma(2),
        ],
        compiler_params=pltpu.CompilerParams(
            collective_id=0, has_side_effects=True, vmem_limit_bytes=56 * 1024 * 1024
        ),
    )(sigma_anc, linear, diag_inverse, pattern)
    hbm = pl.BlockSpec(memory_space=pl.ANY)
    off, diag = pl.pallas_call(
        functools.partial(unpack_kernel, supers, nb),
        out_shape=(
            jax.ShapeDtypeStruct(off.shape, jnp.float32),
            jax.ShapeDtypeStruct((supers, width, width), jnp.float32),
        ),
        in_specs=[vm, vm],
        out_specs=(hbm, hbm),
        scratch_shapes=[f32(supers, width, width), dma(supers * nb + 1)],
        compiler_params=pltpu.CompilerParams(vmem_limit_bytes=8 * 1024 * 1024),
    )(off, res)
    off = jnp.transpose(off.reshape(rows_dev, nb, supers, LANES), (0, 2, 1, 3))
    return off.reshape(anc_factor.shape), diag


def fits(sigma_anc, anc_factor, diag_inverse):
    rows_dev, supers, width = anc_factor.shape
    n_r = lax.axis_size("row")
    n_c = lax.axis_size("col")
    nb = width // LANES
    chunks = (n_r // 2) * n_c * SUBLANES
    return (
        n_r == n_c
        and n_r % 2 == 0
        and supers == 2
        and sigma_anc.shape[0] == sigma_anc.shape[1]
        and diag_inverse.shape[2] % LANES == 0
        and width % (2 * LANES) == 0
        and rows_dev % SUBLANES == 0
        and width % (n_r * n_c * SUBLANES) == 0
        and (nb * (nb + 1) // 2 * LANES) % chunks == 0
    )


def plain_body(sigma_anc, anc_factor, diag_inverse, pattern):
    precise = lax.Precision.HIGHEST
    rows_dev, supers, super_width = anc_factor.shape
    row_count = lax.axis_size("row")
    col_count = lax.axis_size("col")
    position = lax.axis_index("row") * col_count + lax.axis_index("col")
    total_rows = rows_dev * row_count * col_count
    block_size = total_rows // pattern.shape[1]
    flat_mask = jnp.repeat(pattern.astype(jnp.float32), block_size, axis=1)
    own_mask = jnp.transpose(lax.dynamic_slice_in_dim(flat_mask, position * rows_dev, rows_dev, 1))[
        :, :, None
    ]
    device_total = row_count * col_count
    share = -(-super_width // device_total)
    masked_factor = anc_factor * own_mask
    flattened = masked_factor.reshape(rows_dev, -1)
    gathered = lax.all_gather(flattened, "row", axis=0, tiled=True)
    stacked = gathered.reshape(row_count, rows_dev, flattened.shape[1])
    turned = lax.all_to_all(stacked, "col", split_axis=0, concat_axis=1, tiled=True)
    column_block = turned.reshape(row_count * rows_dev, flattened.shape[1])
    summed_rows = lax.psum_scatter(
        jnp.dot(sigma_anc, column_block, precision=precise, preferred_element_type=jnp.float32),
        "col",
        scatter_dimension=0,
        tiled=True,
    )
    off_factor = -(summed_rows.reshape(masked_factor.shape) * own_mask)
    both_rows = jnp.concatenate([masked_factor, off_factor], axis=0)
    column_piece = lax.all_gather(diag_inverse, "row", axis=2, tiled=True)
    product = jnp.einsum("rsk,skj->rsj", both_rows, column_piece, precision=precise)
    own_rows = lax.dynamic_slice_in_dim(column_piece, position * share, share, 1)
    scaled = product[:rows_dev]
    sel_off = product[rows_dev:]
    diag_term = jnp.einsum("skj,skl->sjl", own_rows, own_rows, precision=precise)
    partial_value = diag_term - jnp.einsum("rsj,rsl->sjl", scaled, sel_off, precision=precise)
    sel_diag = lax.psum(partial_value, ("row", "col"))
    return (sel_off, sel_diag)


def body(sigma_anc, anc_factor, diag_inverse, pattern):
    run = fused_body if fits(sigma_anc, anc_factor, diag_inverse) else plain_body
    return run(sigma_anc, anc_factor, diag_inverse, pattern)


def solution(mesh):
    return jax.shard_map(
        body,
        mesh=mesh,
        in_specs=(
            P(("grp", "row"), "col"),
            P(("grp", "row", "col"), None, None),
            P("grp", None, "row"),
            P(),
        ),
        out_specs=(P(("grp", "row", "col"), None, None), P("grp", None, None)),
        check_vma=False,
    )
```

```python
import functools

import jax
import jax.numpy as jnp
from jax import lax
from jax.experimental import pallas as pl
from jax.experimental.pallas import tpu as pltpu
from jax.sharding import PartitionSpec as P

LANES = 128
SUBLANES = 8


def split(x):
    high = x.astype(jnp.bfloat16)
    low = (x - high.astype(jnp.float32)).astype(jnp.bfloat16)
    return high, low


def dot3(a, b, contract=((1,), (0,))):
    (ah, al), (bh, bl) = a, b
    f = lambda u, v: lax.dot_general(u, v, (contract, ((), ())), preferred_element_type=jnp.float32)
    return f(ah, bh) + (f(ah, bl) + f(al, bh))


def columns_of(nb):
    return [[j for j in range(nb) if (j + j // 2) % 2 == core] for core in range(2)]


def pairs_of(nb):
    columns = columns_of(nb)
    pairs = [[], []]
    every = [(i, j) for i in range(nb) for j in range(i + 1)]
    owners = lambda pair: [core for core in range(2) if pair[0] in columns[core] or pair[1] in columns[core]]
    for pair in sorted(every, key=lambda p: len(owners(p))):
        pairs[min(owners(pair), key=lambda core: len(pairs[core]))].append(pair)
    return pairs


def fused_kernel(
    n_r, n_c, supers, width, rows_dev, block_size,
    sig_ref, a_ref, d_ref, pat_ref,
    off_ref, res,
    av, sig_t, wz, sq, dfull, scl, vpart, vrecv, of, offr, gpart, hrecv,
    send_sems, s_w, s_sq, s_sx, s_d, s_scl, s_v, s_off, s_h, s_zag, s_xag, s_sib, local_sems,
):
    r = lax.axis_index("row")
    c = lax.axis_index("col")
    x = r // 2
    k = r % 2
    sib = 2 * x + 1 - k
    par = 2 * (1 - x) + k
    dia = 2 * (1 - x) + 1 - k
    piece = width // n_r
    nb = width // LANES
    half = width // 2
    share = width // n_c
    block_rows = rows_dev * n_c
    columns = columns_of(nb)
    pairs = pairs_of(nb)
    q = len(pairs[0]) * LANES // n_c
    sends = []

    def copy_to(src, dst, rsem, row, col, slot):
        return pltpu.make_async_remote_copy(
            src_ref=src, dst_ref=dst, send_sem=send_sems.at[slot], recv_sem=rsem,
            device_id={"row": row, "col": col}, device_id_type=pl.DeviceIdType.MESH,
        )

    first_slot = 4

    def rcopy(src, dst, rsem, row, col):
        cp = copy_to(src, dst, rsem, row, col, first_slot + len(sends))
        cp.start()
        sends.append(cp)

    def wait_recv(dst, rsem):
        pltpu.make_async_copy(dst, dst, rsem).wait()

    others = [(c + dc) % n_c for dc in range(1, n_c)]
    barrier = pltpu.get_barrier_semaphore()
    sig = lambda row, col: pl.semaphore_signal(
        barrier, inc=1, device_id={"row": row, "col": col}, device_id_type=pl.DeviceIdType.MESH
    )
    for j in others:
        sig(r, j)
    for row in (sib, par, dia):
        sig(row, c)

    def mask_of(first, rows, s):
        row = first + lax.broadcasted_iota(jnp.int32, (rows, 1), 0)
        m = jnp.zeros((rows, 1), jnp.float32)
        for b in range(pat_ref.shape[1]):
            inside = (row >= b * block_size) & (row < (b + 1) * block_size)
            m = jnp.where(inside, pat_ref[s, b].astype(jnp.float32), m)
        return m

    for s in range(supers):
        mask = mask_of((r * n_c + c) * rows_dev, rows_dev, s)
        for t in range(nb):
            rows = a_ref[pl.ds(t * supers + s, rows_dev, stride=nb * supers), :]
            av[s, :, t * LANES : (t + 1) * LANES] = rows * mask
    sig_t[...] = jnp.transpose(sig_ref[...])

    pl.semaphore_wait(barrier, n_c + 2)

    sig_rows = lambda j: pl.ds(pl.multiple_of(j * rows_dev, SUBLANES), rows_dev)
    rcopy(av.at[1 - x], wz.at[1, c], s_w.at[n_c + c], par, c)
    for j in others:
        rcopy(sig_t.at[sig_rows(j), :], sq.at[0, c], s_sq.at[c], r, j)
    for j in others:
        rcopy(av.at[x], wz.at[0, c], s_w.at[c], r, j)
    own_copy = pltpu.make_async_copy(av.at[x], wz.at[0, c], local_sems.at[1])
    own_copy.start()

    d_slice = lambda rr: dfull.at[pl.ds(rr * piece, width - rr * piece), pl.ds(rr * piece, piece)]
    d_src = lambda rr, s: d_ref.at[s, pl.ds(rr * piece, width - rr * piece), :]
    for rr in range(n_r):
        @pl.when(r == rr)
        def _():
            copy_to(d_src(rr, 1 - x), d_slice(rr), s_d.at[rr], par, c, 0).start()
            copy_to(d_src(rr, x), d_slice(rr), s_d.at[rr], sib, c, 1).start()
            pltpu.make_async_copy(d_src(rr, x), d_slice(rr), local_sems.at[0]).start()

    sq[0, c] = sig_t[sig_rows(c), :]
    for rr in range(1, n_r):
        dfull[0 : rr * piece, rr * piece : (rr + 1) * piece] = jnp.zeros((rr * piece, piece), jnp.float32)

    wait_recv(wz.at[1, c], s_w.at[n_c + c])
    for j in others:
        rcopy(wz.at[1, c], wz.at[1, c], s_w.at[n_c + c], r, j)
    for j in others:
        wait_recv(sq.at[0, j], s_sq.at[j])
    rcopy(sq.at[0], sq.at[1], s_sx.at[0], par, c)

    for rr in range(n_r):
        @pl.when(rr == par)
        def _():
            wait_recv(d_slice(rr), s_d.at[rr])
            copy_to(d_slice(rr), d_slice(rr), s_d.at[rr], sib, c, 2).start()
    for rr in range(n_r):
        @pl.when((rr == sib) | (rr == dia))
        def _():
            wait_recv(d_slice(rr), s_d.at[rr])

        @pl.when(rr == r)
        def _():
            pltpu.make_async_copy(d_src(rr, x), d_slice(rr), local_sems.at[0]).wait()

    own_copy.wait()
    near = split(jnp.concatenate([wz[0, c], wz[1, c]], axis=0))
    for j in range(0, width, LANES):
        ds = split(dfull[j:, j : j + LANES])
        v = dot3((near[0][:, j:], near[1][:, j:]), ds)
        scl[r, :, j : j + LANES] = v[:rows_dev]
        scl[par, :, j : j + LANES] = v[rows_dev:]
    rcopy(scl.at[r], scl.at[r], s_scl.at[0], sib, c)
    rcopy(scl.at[par], scl.at[par], s_scl.at[1], sib, c)

    over_rows = ((0,), (0,))
    dz = split(dfull[pl.ds(pl.multiple_of(c * share, SUBLANES), share), :])
    lanes = lambda j: slice(j * LANES, (j + 1) * LANES)
    cut = lambda pair, j: (pair[0][:, lanes(j)], pair[1][:, lanes(j)])
    for core in range(2):
        @pl.when(k == core)
        def _():
            for b, (i, j) in enumerate(pairs[core]):
                gpart[lanes(b), :] = dot3(cut(dz, i), cut(dz, j), over_rows)

    def v_of(side):
        sigma = split(sq[side].reshape(n_r * rows_dev, block_rows))
        return sigma, split(wz[side].reshape(block_rows, width))

    for j in others:
        wait_recv(wz.at[0, j], s_w.at[j])
    vpart[...] = dot3(*v_of(0))
    wait_recv(sq.at[1], s_sx.at[0])
    for j in others:
        wait_recv(wz.at[1, j], s_w.at[n_c + j])
    sigma, ws = v_of(1)
    for h in range(2):
        cols = slice(h * half, (h + 1) * half)
        vpart[:, cols] = vpart[:, cols] + dot3(sigma, (ws[0][:, cols], ws[1][:, cols]))
        rcopy(vpart.at[:, cols], vrecv.at[:, cols], s_v.at[h], sib, c)

    wait_recv(scl.at[sib], s_scl.at[0])
    wait_recv(scl.at[dia], s_scl.at[1])
    all_scl = split(scl[...].reshape(n_r * rows_dev, width))
    mask = jnp.concatenate([mask_of((rr * n_c + c) * rows_dev, rows_dev, x) for rr in range(n_r)], axis=0)
    for h in range(2):
        wait_recv(vrecv.at[:, slice(h * half, (h + 1) * half)], s_v.at[h])
    vs = split((vpart[...] + vrecv[...]) * mask)
    for core in range(2):
        @pl.when(k == core)
        def _():
            ofs = {}
            for slot, j in enumerate(columns[core]):
                at = j * LANES
                v = dot3((vs[0][:, at:], vs[1][:, at:]), split(dfull[at:, at : at + LANES]))
                of[slot] = v.reshape(n_r, rows_dev, LANES)
                ofs[j] = split(v)
            for b, (i, j) in enumerate(pairs[core]):
                left, right = (cut(all_scl, i), ofs[j]) if j in ofs else (ofs[i], cut(all_scl, j))
                gpart[lanes(b), :] += dot3(left, right, over_rows)

    rows_at = lambda j: pl.ds(pl.multiple_of(j * q, SUBLANES), q)
    for j in others:
        rcopy(gpart.at[rows_at(j), :], hrecv.at[c], s_h.at[c], r, j)
    for i, row in enumerate((sib, par, dia)):
        rcopy(of.at[:, row], offr.at[i], s_off.at[i], row, c)

    total = gpart[rows_at(c), :]
    for j in others:
        wait_recv(hrecv.at[j], s_h.at[j])
        total = total + hrecv[j]
    chunk = lambda s, core, j: res.at[s, core, rows_at(j), :]
    res[x, k, rows_at(c), :] = total

    mine = chunk(x, k, c)
    for j in others:
        rcopy(mine, mine, s_zag.at[c], r, j)

    def pass_on(j):
        got = chunk(x, k, j)
        rcopy(got, got, s_xag.at[j], par, c)
        rcopy(got, got, s_sib.at[x * n_c + j], sib, c)

    pass_on(c)

    def put_off(core, s, value):
        for slot, t in enumerate(columns[core]):
            at = pl.ds(t * supers + s, rows_dev, stride=nb * supers)
            off_ref[at, :] = -value(slot)

    for i in range(3):
        wait_recv(offr.at[i], s_off.at[i])
    for core in range(2):
        @pl.when(k == core)
        def _():
            put_off(core, x, lambda slot: of[slot, r])
            put_off(1 - core, x, lambda slot: offr[0, slot])
            put_off(core, 1 - x, lambda slot: offr[1, slot])
            put_off(1 - core, 1 - x, lambda slot: offr[2, slot])

    for j in others:
        wait_recv(chunk(x, k, j), s_zag.at[j])
        pass_on(j)
    for j in [c] + others:
        got = chunk(1 - x, k, j)
        wait_recv(got, s_xag.at[j])
        rcopy(got, got, s_sib.at[(1 - x) * n_c + j], sib, c)
    for s in range(supers):
        for j in range(n_c):
            wait_recv(chunk(s, 1 - k, j), s_sib.at[s * n_c + j])

    for cp in sends:
        cp.wait_send()
    for rr in range(n_r):
        @pl.when(r == rr)
        def _():
            copy_to(d_src(rr, 1 - x), d_slice(rr), s_d.at[rr], par, c, 0).wait_send()
            copy_to(d_src(rr, x), d_slice(rr), s_d.at[rr], sib, c, 1).wait_send()

        @pl.when(rr == par)
        def _():
            copy_to(d_slice(rr), d_slice(rr), s_d.at[rr], sib, c, 2).wait_send()


def unpack_kernel(supers, nb, off_in, res, off_out, diag_out, stage, sems):
    copies = [pltpu.make_async_copy(off_in, off_out, sems.at[supers * nb])]
    copies[0].start()
    place = {pair: (core, b) for core, some in enumerate(pairs_of(nb)) for b, pair in enumerate(some)}
    for s in range(supers):
        for i in range(nb):
            for j in range(nb):
                core, b = place[max(i, j), min(i, j)]
                v = res[s, core, b * LANES : (b + 1) * LANES, :]
                stage[s, i * LANES : (i + 1) * LANES, j * LANES : (j + 1) * LANES] = v if i >= j else jnp.transpose(v)
            at = (s, pl.ds(i * LANES, LANES))
            copies.append(pltpu.make_async_copy(stage.at[at], diag_out.at[at], sems.at[s * nb + i]))
            copies[-1].start()
    for cp in copies:
        cp.wait()


def fused_body(sigma_anc, anc_factor, diag_inverse, pattern):
    rows_dev, supers, width = anc_factor.shape
    n_r = lax.axis_size("row")
    n_c = lax.axis_size("col")
    total_rows = rows_dev * n_r * n_c
    nb = width // LANES
    packed = len(pairs_of(nb)[0]) * LANES
    q = packed // n_c
    slots = len(columns_of(nb)[0])
    f32 = lambda *shape: pltpu.VMEM(shape, jnp.float32)
    dma = lambda n: pltpu.SemaphoreType.DMA((n,))
    vm = pl.BlockSpec(memory_space=pltpu.VMEM)
    linear = jnp.transpose(anc_factor.reshape(rows_dev, supers, nb, LANES), (0, 2, 1, 3))
    linear = linear.reshape(rows_dev * nb * supers, LANES)
    off, res = pl.pallas_call(
        functools.partial(fused_kernel, n_r, n_c, supers, width, rows_dev, total_rows // pattern.shape[1]),
        out_shape=(
            pltpu.VMEM((rows_dev * supers * nb, LANES), jnp.float32),
            pltpu.VMEM((supers, 2, packed, LANES), jnp.float32),
        ),
        in_specs=[vm, vm, vm, pl.BlockSpec(memory_space=pltpu.SMEM)],
        out_specs=(vm, vm),
        scratch_shapes=[
            f32(supers, rows_dev, width),
            f32(n_r * rows_dev, n_c * rows_dev),
            f32(2, n_c, rows_dev, width),
            f32(2, n_c, rows_dev, n_c * rows_dev),
            f32(width, width),
            f32(n_r, rows_dev, width),
            f32(n_r * rows_dev, width),
            f32(n_r * rows_dev, width),
            f32(slots, n_r, rows_dev, LANES),
            f32(3, slots, rows_dev, LANES),
            f32(packed, LANES),
            f32(n_c, q, LANES),
            dma(16 + 12 * n_c),
            dma(2 * n_c), dma(n_c), dma(1), dma(n_r), dma(2), dma(2), dma(3), dma(n_c), dma(n_c), dma(n_c),
            dma(supers * n_c), dma(2),
        ],
        compiler_params=pltpu.CompilerParams(
            collective_id=0, has_side_effects=True, vmem_limit_bytes=48 * 1024 * 1024
        ),
    )(sigma_anc, linear, diag_inverse, pattern)
    hbm = pl.BlockSpec(memory_space=pl.ANY)
    off, diag = pl.pallas_call(
        functools.partial(unpack_kernel, supers, nb),
        out_shape=(
            jax.ShapeDtypeStruct(off.shape, jnp.float32),
            jax.ShapeDtypeStruct((supers, width, width), jnp.float32),
        ),
        in_specs=[vm, vm],
        out_specs=(hbm, hbm),
        scratch_shapes=[f32(supers, width, width), dma(supers * nb + 1)],
        compiler_params=pltpu.CompilerParams(vmem_limit_bytes=8 * 1024 * 1024),
    )(off, res)
    off = jnp.transpose(off.reshape(rows_dev, nb, supers, LANES), (0, 2, 1, 3))
    return off.reshape(anc_factor.shape), diag


def fits(sigma_anc, anc_factor, diag_inverse):
    rows_dev, supers, width = anc_factor.shape
    n_r = lax.axis_size("row")
    n_c = lax.axis_size("col")
    nb = width // LANES
    return (
        n_r == n_c
        and n_r == 2 * supers
        and supers == 2
        and sigma_anc.shape[0] == sigma_anc.shape[1]
        and diag_inverse.shape[2] % LANES == 0
        and nb % 4 == 0
        and rows_dev % SUBLANES == 0
        and width % (n_c * SUBLANES) == 0
        and len(pairs_of(nb)[0]) == len(pairs_of(nb)[1])
        and (len(pairs_of(nb)[0]) * LANES) % (n_c * SUBLANES) == 0
    )


def plain_body(sigma_anc, anc_factor, diag_inverse, pattern):
    precise = lax.Precision.HIGHEST
    rows_dev, supers, super_width = anc_factor.shape
    row_count = lax.axis_size("row")
    col_count = lax.axis_size("col")
    position = lax.axis_index("row") * col_count + lax.axis_index("col")
    total_rows = rows_dev * row_count * col_count
    block_size = total_rows // pattern.shape[1]
    flat_mask = jnp.repeat(pattern.astype(jnp.float32), block_size, axis=1)
    own_mask = jnp.transpose(lax.dynamic_slice_in_dim(flat_mask, position * rows_dev, rows_dev, 1))[
        :, :, None
    ]
    device_total = row_count * col_count
    share = -(-super_width // device_total)
    masked_factor = anc_factor * own_mask
    flattened = masked_factor.reshape(rows_dev, -1)
    gathered = lax.all_gather(flattened, "row", axis=0, tiled=True)
    stacked = gathered.reshape(row_count, rows_dev, flattened.shape[1])
    turned = lax.all_to_all(stacked, "col", split_axis=0, concat_axis=1, tiled=True)
    column_block = turned.reshape(row_count * rows_dev, flattened.shape[1])
    summed_rows = lax.psum_scatter(
        jnp.dot(sigma_anc, column_block, precision=precise, preferred_element_type=jnp.float32),
        "col",
        scatter_dimension=0,
        tiled=True,
    )
    off_factor = -(summed_rows.reshape(masked_factor.shape) * own_mask)
    both_rows = jnp.concatenate([masked_factor, off_factor], axis=0)
    column_piece = lax.all_gather(diag_inverse, "row", axis=2, tiled=True)
    product = jnp.einsum("rsk,skj->rsj", both_rows, column_piece, precision=precise)
    own_rows = lax.dynamic_slice_in_dim(column_piece, position * share, share, 1)
    scaled = product[:rows_dev]
    sel_off = product[rows_dev:]
    diag_term = jnp.einsum("skj,skl->sjl", own_rows, own_rows, precision=precise)
    partial_value = diag_term - jnp.einsum("rsj,rsl->sjl", scaled, sel_off, precision=precise)
    sel_diag = lax.psum(partial_value, ("row", "col"))
    return (sel_off, sel_diag)


def body(sigma_anc, anc_factor, diag_inverse, pattern):
    run = fused_body if fits(sigma_anc, anc_factor, diag_inverse) else plain_body
    return run(sigma_anc, anc_factor, diag_inverse, pattern)


def solution(mesh):
    return jax.shard_map(
        body,
        mesh=mesh,
        in_specs=(
            P(("grp", "row"), "col"),
            P(("grp", "row", "col"), None, None),
            P("grp", None, "row"),
            P(),
        ),
        out_specs=(P(("grp", "row", "col"), None, None), P("grp", None, None)),
        check_vma=False,
    )
```

```python
import functools

import jax
import jax.numpy as jnp
from jax import lax
from jax.experimental import pallas as pl
from jax.experimental.pallas import tpu as pltpu
from jax.sharding import PartitionSpec as P

LANES = 128
SUBLANES = 8


def split(x):
    high = x.astype(jnp.bfloat16)
    low = (x - high.astype(jnp.float32)).astype(jnp.bfloat16)
    return high, low


def dot3(a, b, contract=((1,), (0,))):
    (ah, al), (bh, bl) = a, b
    f = lambda u, v: lax.dot_general(u, v, (contract, ((), ())), preferred_element_type=jnp.float32)
    return f(ah, bh) + (f(ah, bl) + f(al, bh))


def columns_of(nb):
    return [[j for j in range(nb) if (j + j // 2) % 2 == core] for core in range(2)]


def pairs_of(nb):
    columns = columns_of(nb)
    pairs = [[], []]
    every = [(i, j) for i in range(nb) for j in range(i + 1)]
    owners = lambda pair: [core for core in range(2) if pair[0] in columns[core] or pair[1] in columns[core]]
    for pair in sorted(every, key=lambda p: len(owners(p))):
        pairs[min(owners(pair), key=lambda core: len(pairs[core]))].append(pair)
    return pairs


def fused_kernel(
    n_r, n_c, supers, width, rows_dev, block_size,
    sig_hbm, a_hbm, d_ref, pat_ref,
    off_ref, res,
    sig_ref, a_ref, av, sig_t, wz, sq, dfull, scl, vpart, vrecv, of, offr, gpart, hrecv, hjoin, hjrecv,
    send_sems, s_w, s_sq, s_sx, s_d, s_scl, s_v, s_off, s_h, s_hj, s_zag, s_xag, s_far, s_sib, local_sems,
):
    r = lax.axis_index("row")
    c = lax.axis_index("col")
    x = r // 2
    k = r % 2
    sib = 2 * x + 1 - k
    par = 2 * (1 - x) + k
    dia = 2 * (1 - x) + 1 - k
    piece = width // n_r
    nb = width // LANES
    half = width // 2
    share = width // n_c
    block_rows = rows_dev * n_c
    columns = columns_of(nb)
    pairs = pairs_of(nb)
    q = len(pairs[0]) * LANES // n_c
    sends = []

    def copy_to(src, dst, rsem, row, col, slot):
        return pltpu.make_async_remote_copy(
            src_ref=src, dst_ref=dst, send_sem=send_sems.at[slot], recv_sem=rsem,
            device_id={"row": row, "col": col}, device_id_type=pl.DeviceIdType.MESH,
        )

    first_slot = 4
    z_slot = first_slot + 4 * n_c + 12
    done = [0] * (n_c + 1)

    def rcopy(src, dst, rsem, row, col):
        cp = copy_to(src, dst, rsem, row, col, first_slot + len(sends))
        cp.start()
        sends.append(cp)

    plans = [[] for _ in range(n_c)]

    def at_each_col(f):
        for cc in range(n_c):
            pl.when(c == cc)(functools.partial(f, cc))

    def post(cc, refs, row, col):
        slot = z_slot + len(plans[cc])
        make = lambda: copy_to(*refs(), row, col, slot)
        make().start()
        plans[cc].append(make)

    def wait_sends():
        for cp in sends[done[0] :]:
            cp.wait_send()
        done[0] = len(sends)

        def at(cc):
            for make in plans[cc][done[1 + cc] :]:
                make().wait_send()
            done[1 + cc] = len(plans[cc])

        at_each_col(at)

    def giver(j, t):
        edge = j in (0, n_c - 1)
        return j if abs(j - t) == 1 or (edge and abs(j - t) == 2) else t + (1 if j > t else -1)

    by_distance = lambda cc: sorted((j for j in range(n_c) if j != cc), key=lambda j: abs(j - cc))

    def wait_recv(dst, rsem):
        pltpu.make_async_copy(dst, dst, rsem).wait()

    loads = [
        pltpu.make_async_copy(a_hbm, a_ref, local_sems.at[2]),
        pltpu.make_async_copy(sig_hbm, sig_ref, local_sems.at[3]),
    ]
    for cp in loads:
        cp.start()
    others = [(c + dc) % n_c for dc in range(1, n_c)]
    barrier = pltpu.get_barrier_semaphore()
    sig = lambda row, col: pl.semaphore_signal(
        barrier, inc=1, device_id={"row": row, "col": col}, device_id_type=pl.DeviceIdType.MESH
    )
    for j in others:
        sig(r, j)
    for row in (sib, par, dia):
        sig(row, c)

    def mask_of(first, rows, s):
        row = first + lax.broadcasted_iota(jnp.int32, (rows, 1), 0)
        m = jnp.zeros((rows, 1), jnp.float32)
        for b in range(pat_ref.shape[1]):
            inside = (row >= b * block_size) & (row < (b + 1) * block_size)
            m = jnp.where(inside, pat_ref[s, b].astype(jnp.float32), m)
        return m

    loads[0].wait()
    for s in range(supers):
        mask = mask_of((r * n_c + c) * rows_dev, rows_dev, s)
        for t in range(nb):
            rows = a_ref[pl.ds(t * supers + s, rows_dev, stride=nb * supers), :]
            av[s, :, t * LANES : (t + 1) * LANES] = rows * mask
    loads[1].wait()
    sig_t[...] = jnp.transpose(sig_ref[...])

    pl.semaphore_wait(barrier, n_c + 2)

    sig_rows = lambda j: pl.ds(pl.multiple_of(j * rows_dev, SUBLANES), rows_dev)
    rcopy(av.at[1 - x], wz.at[1, c], s_w.at[n_c + c], par, c)

    row_block = lambda side, j: (wz.at[side, j], s_w.at[side * n_c + j])

    def spread(cc, src, side):
        for t in by_distance(cc):
            if giver(cc, t) == cc:
                post(cc, lambda: (src(), *row_block(side, cc)), r, t)

    def pass_rows(cc, side, upto):
        for j in by_distance(cc):
            if (abs(j - cc) == 1) == upto:
                wait_recv(*row_block(side, j))
                for t in range(n_c):
                    if t not in (j, cc) and giver(j, t) == cc:
                        post(cc, lambda j=j: (wz.at[side, j], *row_block(side, j)), r, t)

    def send_first(cc):
        for j in by_distance(cc):
            post(cc, lambda j=j: (sig_t.at[sig_rows(j), :], sq.at[0, cc], s_sq.at[cc]), r, j)
        spread(cc, lambda: av.at[x], 0)

    at_each_col(send_first)
    own_copy = pltpu.make_async_copy(av.at[x], wz.at[0, c], local_sems.at[1])
    own_copy.start()

    d_slice = lambda rr: dfull.at[pl.ds(rr * piece, width - rr * piece), pl.ds(rr * piece, piece)]
    d_src = lambda rr, s: d_ref.at[s, pl.ds(rr * piece, width - rr * piece), :]
    for rr in range(n_r):
        @pl.when(r == rr)
        def _():
            copy_to(d_src(rr, 1 - x), d_slice(rr), s_d.at[rr], par, c, 0).start()
            copy_to(d_src(rr, x), d_slice(rr), s_d.at[rr], sib, c, 1).start()
            pltpu.make_async_copy(d_src(rr, x), d_slice(rr), local_sems.at[0]).start()

    sq[0, c] = sig_t[sig_rows(c), :]
    for rr in range(1, n_r):
        dfull[0 : rr * piece, rr * piece : (rr + 1) * piece] = jnp.zeros((rr * piece, piece), jnp.float32)

    wait_recv(wz.at[1, c], s_w.at[n_c + c])
    at_each_col(lambda cc: spread(cc, lambda: wz.at[1, cc], 1))
    for j in others:
        wait_recv(sq.at[0, j], s_sq.at[j])
    rcopy(sq.at[0], sq.at[1], s_sx.at[0], par, c)
    at_each_col(lambda cc: pass_rows(cc, 0, True))
    at_each_col(lambda cc: pass_rows(cc, 0, False))

    for rr in range(n_r):
        @pl.when(rr == par)
        def _():
            wait_recv(d_slice(rr), s_d.at[rr])
            copy_to(d_slice(rr), d_slice(rr), s_d.at[rr], sib, c, 2).start()
    at_each_col(lambda cc: pass_rows(cc, 1, True))
    for rr in range(n_r):
        @pl.when((rr == sib) | (rr == dia))
        def _():
            wait_recv(d_slice(rr), s_d.at[rr])

        @pl.when(rr == r)
        def _():
            pltpu.make_async_copy(d_src(rr, x), d_slice(rr), local_sems.at[0]).wait()

    own_copy.wait()
    near = split(jnp.concatenate([wz[0, c], wz[1, c]], axis=0))
    for j in range(0, width, LANES):
        ds = split(dfull[j:, j : j + LANES])
        v = dot3((near[0][:, j:], near[1][:, j:]), ds)
        scl[r, :, j : j + LANES] = v[:rows_dev]
        scl[par, :, j : j + LANES] = v[rows_dev:]
    rcopy(scl.at[r], scl.at[r], s_scl.at[0], sib, c)
    rcopy(scl.at[par], scl.at[par], s_scl.at[1], sib, c)

    over_rows = ((0,), (0,))
    dz = split(dfull[pl.ds(pl.multiple_of(c * share, SUBLANES), share), :])
    lanes = lambda j: slice(j * LANES, (j + 1) * LANES)
    cut = lambda pair, j: (pair[0][:, lanes(j)], pair[1][:, lanes(j)])
    for core in range(2):
        @pl.when(k == core)
        def _():
            for b, (i, j) in enumerate(pairs[core]):
                gpart[lanes(b), :] = dot3(cut(dz, i), cut(dz, j), over_rows)

    def v_of(side):
        sigma = split(sq[side].reshape(n_r * rows_dev, block_rows))
        return sigma, split(wz[side].reshape(block_rows, width))

    vpart[...] = dot3(*v_of(0))
    wait_recv(sq.at[1], s_sx.at[0])
    at_each_col(lambda cc: pass_rows(cc, 1, False))
    sigma, ws = v_of(1)
    for h in range(2):
        cols = slice(h * half, (h + 1) * half)
        vpart[:, cols] = vpart[:, cols] + dot3(sigma, (ws[0][:, cols], ws[1][:, cols]))
        rcopy(vpart.at[:, cols], vrecv.at[:, cols], s_v.at[h], sib, c)

    wait_recv(scl.at[sib], s_scl.at[0])
    wait_recv(scl.at[dia], s_scl.at[1])
    all_scl = split(scl[...].reshape(n_r * rows_dev, width))
    mask = jnp.concatenate([mask_of((rr * n_c + c) * rows_dev, rows_dev, x) for rr in range(n_r)], axis=0)
    for h in range(2):
        wait_recv(vrecv.at[:, slice(h * half, (h + 1) * half)], s_v.at[h])
    vs = split((vpart[...] + vrecv[...]) * mask)
    for core in range(2):
        @pl.when(k == core)
        def _():
            ofs = {}
            for slot, j in enumerate(columns[core]):
                at = j * LANES
                v = dot3((vs[0][:, at:], vs[1][:, at:]), split(dfull[at:, at : at + LANES]))
                of[slot] = v.reshape(n_r, rows_dev, LANES)
                ofs[j] = split(v)
            for b, (i, j) in enumerate(pairs[core]):
                left, right = (cut(all_scl, i), ofs[j]) if j in ofs else (ofs[i], cut(all_scl, j))
                gpart[lanes(b), :] += dot3(left, right, over_rows)

    rows_at = lambda j: pl.ds(pl.multiple_of(j * q, SUBLANES), q)

    joined = lambda j, t: j in (0, n_c - 1) and abs(j - t) == 2

    def scatter(cc):
        targets = sorted((t for t in range(n_c) if t != cc), key=lambda t: (not joined(cc, t), -abs(t - cc)))
        late = [t for t in targets if any(joined(j, t) and (j + t) // 2 == cc for j in range(n_c))]
        for t in targets:
            if joined(cc, t):
                post(cc, lambda t=t: (gpart.at[rows_at(t), :], hrecv.at[t], s_h.at[t]), r, (cc + t) // 2)
            elif t not in late:
                post(cc, lambda t=t: (gpart.at[rows_at(t), :], hrecv.at[cc], s_h.at[cc]), r, t)
        for t in late:
            wait_recv(hrecv.at[t], s_h.at[t])
            hjoin[...] = gpart[rows_at(t), :] + hrecv[t]
            post(cc, lambda: (hjoin, hjrecv, s_hj.at[0]), r, t)

    at_each_col(scatter)
    for i, row in enumerate((sib, par, dia)):
        rcopy(of.at[:, row], offr.at[i], s_off.at[i], row, c)

    wait_sends()
    mine_at = lambda: gpart.at[rows_at(c), :]

    def collect(cc):
        for j in by_distance(cc):
            if joined(j, cc):
                continue
            if any(joined(i, cc) and (i + cc) // 2 == j for i in range(n_c)):
                wait_recv(hjrecv, s_hj.at[0])
                mine_at()[...] += hjrecv[...]
            else:
                wait_recv(hrecv.at[j], s_h.at[j])
                mine_at()[...] += hrecv[j]

    at_each_col(collect)
    total = gpart[rows_at(c), :]
    chunk = lambda s, core, j: res.at[s, core, rows_at(j), :]
    res[x, k, rows_at(c), :] = total

    mine = chunk(x, k, c)
    rcopy(mine, mine, s_xag.at[c], par, c)

    def gather(cc):
        for t in by_distance(cc):
            if giver(cc, t) == cc:
                post(cc, lambda: (chunk(x, k, cc), chunk(x, k, cc), s_zag.at[cc]), r, t)

    at_each_col(gather)
    rcopy(mine, mine, s_sib.at[x * n_c + c], sib, c)
    opposite = n_c - 1 - c

    def put_off(core, s, value):
        for slot, t in enumerate(columns[core]):
            at = pl.ds(t * supers + s, rows_dev, stride=nb * supers)
            off_ref[at, :] = -value(slot)

    for i in range(3):
        wait_recv(offr.at[i], s_off.at[i])
    for core in range(2):
        @pl.when(k == core)
        def _():
            put_off(core, x, lambda slot: of[slot, r])
            put_off(1 - core, x, lambda slot: offr[0, slot])
            put_off(core, 1 - x, lambda slot: offr[1, slot])
            put_off(1 - core, 1 - x, lambda slot: offr[2, slot])

    away = 1 - x
    theirs = chunk(away, k, c)
    wait_recv(theirs, s_xag.at[c])
    rcopy(theirs, theirs, s_far.at[c], r, opposite)
    rcopy(theirs, theirs, s_sib.at[(1 - x) * n_c + c], sib, c)

    def pass_on(cc):
        for j in by_distance(cc):
            got = chunk(x, k, j)
            wait_recv(got, s_zag.at[j])
            for t in range(n_c):
                if t not in (j, cc) and giver(j, t) == cc:
                    post(cc, lambda j=j: (chunk(x, k, j), chunk(x, k, j), s_zag.at[j]), r, t)
            if j != n_c - 1 - cc:
                forward(cc, x, j, lambda j=j: s_xag.at[j], par)
            forward(cc, x, j, lambda j=j: s_sib.at[x * n_c + j], sib)
        for j in by_distance(cc):
            got = chunk(1 - x, k, j)
            wait_recv(got, s_far.at[j] if j == n_c - 1 - cc else s_xag.at[j])
            forward(cc, away, j, lambda j=j: s_sib.at[away * n_c + j], sib)

    def forward(cc, s, j, rsem, row):
        post(cc, lambda: (chunk(s, k, j), chunk(s, k, j), rsem()), row, c)

    at_each_col(pass_on)
    for s in range(supers):
        for j in range(n_c):
            wait_recv(chunk(s, 1 - k, j), s_sib.at[s * n_c + j])

    wait_sends()
    for rr in range(n_r):
        @pl.when(r == rr)
        def _():
            copy_to(d_src(rr, 1 - x), d_slice(rr), s_d.at[rr], par, c, 0).wait_send()
            copy_to(d_src(rr, x), d_slice(rr), s_d.at[rr], sib, c, 1).wait_send()

        @pl.when(rr == par)
        def _():
            copy_to(d_slice(rr), d_slice(rr), s_d.at[rr], sib, c, 2).wait_send()


def unpack_kernel(supers, nb, off_in, res, off_out, diag_out, stage, sems):
    copies = [pltpu.make_async_copy(off_in, off_out, sems.at[supers * nb])]
    copies[0].start()
    place = {pair: (core, b) for core, some in enumerate(pairs_of(nb)) for b, pair in enumerate(some)}
    for s in range(supers):
        for i in range(nb):
            for j in range(nb):
                core, b = place[max(i, j), min(i, j)]
                v = res[s, core, b * LANES : (b + 1) * LANES, :]
                stage[s, i * LANES : (i + 1) * LANES, j * LANES : (j + 1) * LANES] = v if i >= j else jnp.transpose(v)
            at = (s, pl.ds(i * LANES, LANES))
            copies.append(pltpu.make_async_copy(stage.at[at], diag_out.at[at], sems.at[s * nb + i]))
            copies[-1].start()
    for cp in copies:
        cp.wait()


def fused_body(sigma_anc, anc_factor, diag_inverse, pattern):
    rows_dev, supers, width = anc_factor.shape
    n_r = lax.axis_size("row")
    n_c = lax.axis_size("col")
    total_rows = rows_dev * n_r * n_c
    nb = width // LANES
    packed = len(pairs_of(nb)[0]) * LANES
    q = packed // n_c
    slots = len(columns_of(nb)[0])
    f32 = lambda *shape: pltpu.VMEM(shape, jnp.float32)
    dma = lambda n: pltpu.SemaphoreType.DMA((n,))
    vm = pl.BlockSpec(memory_space=pltpu.VMEM)
    linear = jnp.transpose(anc_factor.reshape(rows_dev, supers, nb, LANES), (0, 2, 1, 3))
    linear = linear.reshape(rows_dev * nb * supers, LANES)
    hbm = pl.BlockSpec(memory_space=pl.ANY)
    off, res = pl.pallas_call(
        functools.partial(fused_kernel, n_r, n_c, supers, width, rows_dev, total_rows // pattern.shape[1]),
        out_shape=(
            pltpu.VMEM((rows_dev * supers * nb, LANES), jnp.float32),
            pltpu.VMEM((supers, 2, packed, LANES), jnp.float32),
        ),
        in_specs=[hbm, hbm, hbm, pl.BlockSpec(memory_space=pltpu.SMEM)],
        out_specs=(vm, vm),
        scratch_shapes=[
            f32(*sigma_anc.shape),
            f32(*linear.shape),
            f32(supers, rows_dev, width),
            f32(n_r * rows_dev, n_c * rows_dev),
            f32(2, n_c, rows_dev, width),
            f32(2, n_c, rows_dev, n_c * rows_dev),
            f32(width, width),
            f32(n_r, rows_dev, width),
            f32(n_r * rows_dev, width),
            f32(n_r * rows_dev, width),
            f32(slots, n_r, rows_dev, LANES),
            f32(3, slots, rows_dev, LANES),
            f32(packed, LANES),
            f32(n_c, q, LANES),
            f32(q, LANES),
            f32(q, LANES),
            dma(16 + 24 * n_c),
            dma(2 * n_c), dma(n_c), dma(1), dma(n_r), dma(2), dma(2), dma(3), dma(n_c), dma(1), dma(n_c), dma(n_c), dma(n_c),
            dma(supers * n_c), dma(4),
        ],
        compiler_params=pltpu.CompilerParams(
            collective_id=0, has_side_effects=True, vmem_limit_bytes=58 * 1024 * 1024
        ),
    )(sigma_anc, linear, diag_inverse, pattern)
    off, diag = pl.pallas_call(
        functools.partial(unpack_kernel, supers, nb),
        out_shape=(
            jax.ShapeDtypeStruct(off.shape, jnp.float32),
            jax.ShapeDtypeStruct((supers, width, width), jnp.float32),
        ),
        in_specs=[vm, vm],
        out_specs=(hbm, hbm),
        scratch_shapes=[f32(supers, width, width), dma(supers * nb + 1)],
        compiler_params=pltpu.CompilerParams(vmem_limit_bytes=8 * 1024 * 1024),
    )(off, res)
    off = jnp.transpose(off.reshape(rows_dev, nb, supers, LANES), (0, 2, 1, 3))
    return off.reshape(anc_factor.shape), diag


def fits(sigma_anc, anc_factor, diag_inverse):
    rows_dev, supers, width = anc_factor.shape
    n_r = lax.axis_size("row")
    n_c = lax.axis_size("col")
    nb = width // LANES
    return (
        n_r == n_c
        and n_r == 2 * supers
        and supers == 2
        and sigma_anc.shape[0] == sigma_anc.shape[1]
        and diag_inverse.shape[2] % LANES == 0
        and nb % 4 == 0
        and rows_dev % SUBLANES == 0
        and width % (n_c * SUBLANES) == 0
        and len(pairs_of(nb)[0]) == len(pairs_of(nb)[1])
        and (len(pairs_of(nb)[0]) * LANES) % (n_c * SUBLANES) == 0
    )


def plain_body(sigma_anc, anc_factor, diag_inverse, pattern):
    precise = lax.Precision.HIGHEST
    rows_dev, supers, super_width = anc_factor.shape
    row_count = lax.axis_size("row")
    col_count = lax.axis_size("col")
    position = lax.axis_index("row") * col_count + lax.axis_index("col")
    total_rows = rows_dev * row_count * col_count
    block_size = total_rows // pattern.shape[1]
    flat_mask = jnp.repeat(pattern.astype(jnp.float32), block_size, axis=1)
    own_mask = jnp.transpose(lax.dynamic_slice_in_dim(flat_mask, position * rows_dev, rows_dev, 1))[
        :, :, None
    ]
    device_total = row_count * col_count
    share = -(-super_width // device_total)
    masked_factor = anc_factor * own_mask
    flattened = masked_factor.reshape(rows_dev, -1)
    gathered = lax.all_gather(flattened, "row", axis=0, tiled=True)
    stacked = gathered.reshape(row_count, rows_dev, flattened.shape[1])
    turned = lax.all_to_all(stacked, "col", split_axis=0, concat_axis=1, tiled=True)
    column_block = turned.reshape(row_count * rows_dev, flattened.shape[1])
    summed_rows = lax.psum_scatter(
        jnp.dot(sigma_anc, column_block, precision=precise, preferred_element_type=jnp.float32),
        "col",
        scatter_dimension=0,
        tiled=True,
    )
    off_factor = -(summed_rows.reshape(masked_factor.shape) * own_mask)
    both_rows = jnp.concatenate([masked_factor, off_factor], axis=0)
    column_piece = lax.all_gather(diag_inverse, "row", axis=2, tiled=True)
    product = jnp.einsum("rsk,skj->rsj", both_rows, column_piece, precision=precise)
    own_rows = lax.dynamic_slice_in_dim(column_piece, position * share, share, 1)
    scaled = product[:rows_dev]
    sel_off = product[rows_dev:]
    diag_term = jnp.einsum("skj,skl->sjl", own_rows, own_rows, precision=precise)
    partial_value = diag_term - jnp.einsum("rsj,rsl->sjl", scaled, sel_off, precision=precise)
    sel_diag = lax.psum(partial_value, ("row", "col"))
    return (sel_off, sel_diag)


def body(sigma_anc, anc_factor, diag_inverse, pattern):
    run = fused_body if fits(sigma_anc, anc_factor, diag_inverse) else plain_body
    return run(sigma_anc, anc_factor, diag_inverse, pattern)


def solution(mesh):
    return jax.shard_map(
        body,
        mesh=mesh,
        in_specs=(
            P(("grp", "row"), "col"),
            P(("grp", "row", "col"), None, None),
            P("grp", None, "row"),
            P(),
        ),
        out_specs=(P(("grp", "row", "col"), None, None), P("grp", None, None)),
        check_vma=False,
    )
```

```python
import functools

import jax
import jax.numpy as jnp
from jax import lax
from jax.experimental import pallas as pl
from jax.experimental.pallas import tpu as pltpu
from jax.sharding import PartitionSpec as P

LANES = 128
SUBLANES = 8
PARTS = 4


def split(x):
    high = x.astype(jnp.bfloat16)
    low = (x - high.astype(jnp.float32)).astype(jnp.bfloat16)
    return high, low


def dot3(a, b, contract=((1,), (0,))):
    (ah, al), (bh, bl) = a, b
    f = lambda u, v: lax.dot_general(u, v, (contract, ((), ())), preferred_element_type=jnp.float32)
    return f(ah, bh) + (f(ah, bl) + f(al, bh))


def columns_of(nb):
    return [[j for j in range(nb) if (j + j // 2) % 2 == core] for core in range(2)]


def pairs_of(nb):
    columns = columns_of(nb)
    pairs = [[], []]
    every = [(i, j) for i in range(nb) for j in range(i + 1)]
    owners = lambda pair: [core for core in range(2) if pair[0] in columns[core] or pair[1] in columns[core]]
    for pair in sorted(every, key=lambda p: len(owners(p))):
        pairs[min(owners(pair), key=lambda core: len(pairs[core]))].append(pair)
    return pairs


def fused_kernel(
    n_r, n_c, supers, width, rows_dev, block_size, parts,
    sig_hbm, a_hbm, d_ref, pat_ref,
    off_ref, res,
    sig_ref, a_ref, av, sig_t, wz, sq, dfull, scl, vpart, vrecv, of, offr, gpart, grecv,
    send_sems, s_w, s_sq, s_d, s_scl, s_v, s_off, s_h, s_g, s_sib, local_sems,
):
    r = lax.axis_index("row")
    c = lax.axis_index("col")
    x = r // 2
    k = r % 2
    away = 1 - x
    sib = 2 * x + 1 - k
    par = 2 * away + k
    dia = 2 * away + 1 - k
    piece = width // n_r
    nb = width // LANES
    block_rows = rows_dev * n_c
    side_rows = 2 * rows_dev
    columns = columns_of(nb)
    pairs = pairs_of(nb)
    q = len(pairs[0]) * LANES // (2 * parts)
    low = n_c // 2 - 1
    side = c // 2
    mate = 4 * side + 1 - c
    hub = low + side
    is_hub = hub == c
    is_edge = hub != c
    plans = [[] for _ in range(n_c)]
    done = [0] * n_c
    v_slot = 4
    z_slot = v_slot + nb

    def copy_to(src, dst, rsem, row, col, slot):
        return pltpu.make_async_remote_copy(
            src_ref=src, dst_ref=dst, send_sem=send_sems.at[slot], recv_sem=rsem,
            device_id={"row": row, "col": col}, device_id_type=pl.DeviceIdType.MESH,
        )

    def at_each_col(hub_part, edge_part=None):
        for cc in range(n_c):
            hub_col = low + cc // 2
            part = hub_part if cc == hub_col else edge_part
            if part is not None:
                pl.when(c == cc)(functools.partial(part, cc, n_c - 1 - cc))

    def post(cc, refs, row, col):
        slot = z_slot + len(plans[cc])
        make = lambda: copy_to(*refs(), row, col, slot)
        make().start()
        plans[cc].append(make)

    def wait_sends():
        def at(cc, *_):
            for make in plans[cc][done[cc] :]:
                make().wait_send()
            done[cc] = len(plans[cc])

        at_each_col(at, at)

    def wait_recv(dst, rsem):
        pltpu.make_async_copy(dst, dst, rsem).wait()

    loads = [
        pltpu.make_async_copy(a_hbm, a_ref, local_sems.at[2]),
        pltpu.make_async_copy(sig_hbm, sig_ref, local_sems.at[3]),
    ]
    for cp in loads:
        cp.start()
    barrier = pltpu.get_barrier_semaphore()
    sig = lambda row, col: pl.semaphore_signal(
        barrier, inc=1, device_id={"row": row, "col": col}, device_id_type=pl.DeviceIdType.MESH
    )
    for dc in range(1, n_c):
        sig(r, (c + dc) % n_c)
    for row in (sib, par, dia):
        sig(row, c)
        sig(row, mate)

    def mask_of(first, rows, s):
        row = first + lax.broadcasted_iota(jnp.int32, (rows, 1), 0)
        m = jnp.zeros((rows, 1), jnp.float32)
        for b in range(pat_ref.shape[1]):
            inside = (row >= b * block_size) & (row < (b + 1) * block_size)
            m = jnp.where(inside, pat_ref[s, b].astype(jnp.float32), m)
        return m

    loads[0].wait()
    for s in range(supers):
        mask = mask_of((r * n_c + c) * rows_dev, rows_dev, s)
        for t in range(nb):
            rows = a_ref[pl.ds(t * supers + s, rows_dev, stride=nb * supers), :]
            av[s, :, t * LANES : (t + 1) * LANES] = rows * mask
    loads[1].wait()
    sig_t[...] = jnp.transpose(sig_ref[...])

    pl.semaphore_wait(barrier, n_c + 5)

    rows_w = lambda own, j: (wz.at[own, j], s_w.at[own * n_c + j])
    rows_s = lambda own, j: (sq.at[own, j], s_sq.at[own * n_c + j])
    half_of = lambda h: sig_t.at[pl.ds(h * side_rows, side_rows), :]
    d_slice = lambda rr: dfull.at[pl.ds(rr * piece, width - rr * piece), pl.ds(rr * piece, piece)]
    d_src = lambda rr, s: d_ref.at[s, pl.ds(rr * piece, width - rr * piece), :]
    sends_d = (is_hub & (k == 0)) | (is_edge & (k == 1))

    def hub_first(cc, other):
        post(cc, lambda: (av.at[away], *rows_w(1, cc)), par, c)
        post(cc, lambda: (half_of(1 - cc // 2), *rows_s(0, cc)), r, other)
        post(cc, lambda: (av.at[x], *rows_w(0, cc)), r, other)
        post(cc, lambda: (half_of(cc // 2), *rows_s(1, cc)), par, c)

    def edge_first(cc, other):
        near = low + cc // 2
        post(cc, lambda: (av.at[away], *rows_w(1, cc)), par, c)
        post(cc, lambda: (av.at[x], *rows_w(0, cc)), r, near)
        post(cc, lambda: (half_of(1 - cc // 2), *rows_s(0, cc)), r, n_c - 1 - near)
        post(cc, lambda: (half_of(cc // 2), *rows_s(0, cc)), r, near)

    at_each_col(hub_first, edge_first)
    for rr in range(n_r):
        @pl.when((r == rr) & sends_d)
        def _():
            copy_to(d_src(rr, away), d_slice(rr), s_d.at[rr], par, c, 0).start()

        @pl.when((r == rr) & is_hub)
        def _():
            copy_to(d_src(rr, x), d_slice(rr), s_d.at[rr], sib, c, 1).start()
            pltpu.make_async_copy(d_src(rr, x), d_slice(rr), local_sems.at[0]).start()

    @pl.when(is_hub)
    def _():
        wz[0, c] = av[x]
        sq[0, c] = sig_t[pl.ds(pl.multiple_of(side * side_rows, SUBLANES), side_rows), :]
        for rr in range(1, n_r):
            dfull[0 : rr * piece, rr * piece : (rr + 1) * piece] = jnp.zeros((rr * piece, piece), jnp.float32)

    def hub_pass(cc, other):
        edge = 0 if cc == low else n_c - 1
        wait_recv(*rows_w(1, cc))
        post(cc, lambda: (wz.at[1, cc], *rows_w(1, cc)), r, other)
        wait_recv(*rows_w(0, edge))
        post(cc, lambda: (wz.at[0, edge], *rows_w(0, edge)), r, other)
        for j in (other, edge, n_c - 1 - edge):
            wait_recv(*rows_s(0, j))
            post(cc, lambda j=j: (sq.at[0, j], *rows_s(1, j)), par, c)

    def hub_pass_last(cc, other):
        edge = 0 if cc == low else n_c - 1
        wait_recv(*rows_w(1, edge))
        post(cc, lambda: (wz.at[1, edge], *rows_w(1, edge)), r, other)

    def edge_pass(cc, other):
        wait_recv(*rows_w(1, cc))
        post(cc, lambda: (wz.at[1, cc], *rows_w(1, cc)), r, low + cc // 2)

    at_each_col(hub_pass, edge_pass)
    for rr in range(n_r):
        @pl.when((rr == par) & is_hub)
        def _():
            @pl.when(k == 0)
            def _():
                wait_recv(d_slice(rr), s_d.at[rr])
                copy_to(d_slice(rr), d_slice(rr), s_d.at[rr], sib, c, 2).start()

        @pl.when((rr == par) & is_edge & (k == 1))
        def _():
            wait_recv(d_slice(rr), s_d.at[rr])
            copy_to(d_slice(rr), d_slice(rr), s_d.at[rr], r, hub, 3).start()
    at_each_col(hub_pass_last)
    for rr in range(n_r):
        @pl.when((rr == par) & is_hub & (k == 1))
        def _():
            wait_recv(d_slice(rr), s_d.at[rr])
            copy_to(d_slice(rr), d_slice(rr), s_d.at[rr], sib, c, 2).start()
    for rr in range(n_r):
        @pl.when(((rr == sib) | (rr == dia)) & is_hub)
        def _():
            wait_recv(d_slice(rr), s_d.at[rr])

        @pl.when((rr == r) & is_hub)
        def _():
            pltpu.make_async_copy(d_src(rr, x), d_slice(rr), local_sems.at[0]).wait()

    over_rows = ((0,), (0,))
    lanes = lambda j: slice(j * LANES, (j + 1) * LANES)
    cut = lambda pair, j: (pair[0][:, lanes(j)], pair[1][:, lanes(j)])
    mask_rows = lambda: jnp.concatenate(
        [mask_of((rr * n_c + 2 * side) * rows_dev, side_rows, x) for rr in range(n_r)], axis=0
    )

    @pl.when(is_hub)
    def _():
        own = [wz[o, pl.ds(2 * side, 2)].reshape(side_rows, width) for o in range(2)]
        near = split(jnp.concatenate(own, axis=0))
        for j in range(0, width, LANES):
            ds = split(dfull[j:, j : j + LANES])
            v = dot3((near[0][:, j:], near[1][:, j:]), ds)
            scl[r, :, j : j + LANES] = v[:side_rows]
            scl[par, :, j : j + LANES] = v[side_rows:]

    def hub_scl(cc, *_):
        post(cc, lambda: (scl.at[r], scl.at[r], s_scl.at[0]), sib, c)
        post(cc, lambda: (scl.at[par], scl.at[par], s_scl.at[1]), sib, c)

    at_each_col(hub_scl)

    @pl.when(is_hub)
    def _():
        dz = split(dfull[pl.ds(pl.multiple_of(side * (width // 2), SUBLANES), width // 2), :])
        for core in range(2):
            @pl.when(k == core)
            def _():
                for b, (i, j) in enumerate(pairs[core]):
                    gpart[lanes(b), :] = dot3(cut(dz, i), cut(dz, j), over_rows)

    def v_of(own):
        sigma = split(sq[own].reshape(n_r * side_rows, block_rows))
        return sigma, split(wz[own].reshape(block_rows, width))

    def hub_wait(own, cc, other):
        edge = 0 if cc == low else n_c - 1
        for j in (other, n_c - 1 - edge):
            wait_recv(*rows_w(own, j))
        if own == 1:
            for j in range(n_c):
                wait_recv(*rows_s(1, j))

    at_each_col(functools.partial(hub_wait, 0))

    @pl.when(is_hub)
    def _():
        vpart[...] = dot3(*v_of(0))

    at_each_col(functools.partial(hub_wait, 1))
    v_cols = lambda h: slice(h * LANES, (h + 1) * LANES)

    @pl.when(is_hub)
    def _():
        sigma, ws = v_of(1)
        for h in range(nb):
            vpart[:, v_cols(h)] = vpart[:, v_cols(h)] + dot3(sigma, cut(ws, h))
            copy_to(vpart.at[:, v_cols(h)], vrecv.at[:, v_cols(h)], s_v.at[h], sib, c, v_slot + h).start()

        wait_recv(scl.at[sib], s_scl.at[0])
        wait_recv(scl.at[dia], s_scl.at[1])
        all_scl = split(scl[...].reshape(n_r * side_rows, width))
        for h in range(nb):
            wait_recv(vrecv.at[:, v_cols(h)], s_v.at[h])
        vs = split((vpart[...] + vrecv[...]) * mask_rows())
        for core in range(2):
            @pl.when(k == core)
            def _():
                ofs = {}
                for slot, j in enumerate(columns[core]):
                    at = j * LANES
                    v = dot3((vs[0][:, at:], vs[1][:, at:]), split(dfull[at:, at : at + LANES]))
                    of[slot] = v.reshape(n_r, 2, rows_dev, LANES)
                    ofs[j] = split(v)
                for b, (i, j) in enumerate(pairs[core]):
                    left, right = (cut(all_scl, i), ofs[j]) if j in ofs else (ofs[i], cut(all_scl, j))
                    gpart[lanes(b), :] += dot3(left, right, over_rows)

    rows_at = lambda h, i: pl.ds((h * parts + i) * q, q)
    chunk = lambda s, h, i: (res.at[s, k, rows_at(h, i), :], s_g.at[(s * 2 + h) * parts + i])
    held = lambda s, h, i: res.at[s, k, rows_at(h, i), :]

    def hub_scatter(cc, other):
        for i in range(parts):
            post(cc, lambda i=i: (gpart.at[rows_at(1 - cc // 2, i), :], grecv.at[i], s_h.at[i]), r, other)
        edge = 0 if cc == low else n_c - 1
        for row in (sib, par, dia):
            post(cc, lambda row=row: (of.at[:, row, cc - 2 * (cc // 2)], offr.at[r], s_off.at[r]), row, cc)
        for row in (r, sib, par, dia):
            post(cc, lambda row=row: (of.at[:, row, edge - 2 * (cc // 2)], offr.at[r], s_off.at[r]), row, edge)
        pltpu.make_async_copy(of.at[:, r, cc - 2 * (cc // 2)], offr.at[r], s_off.at[r]).start()

    at_each_col(hub_scatter)
    wait_sends()

    def forward(cc, s, h, i, row, col):
        post(cc, lambda: (held(s, h, i), *chunk(s, h, i)), row, col)

    def to_sib(cc, s, h, i):
        post(cc, lambda: (held(s, h, i), held(s, h, i), s_sib.at[(s * 2 + h) * parts + i]), sib, c)

    def hub_reduce(cc, other):
        h = cc // 2
        edge = 0 if cc == low else n_c - 1
        for i in range(parts):
            wait_recv(grecv.at[i], s_h.at[i])
            res[x, k, rows_at(h, i), :] = gpart[rows_at(h, i), :] + grecv[i]
            forward(cc, x, h, i, par, c)
            forward(cc, x, h, i, r, other)
            forward(cc, x, h, i, r, edge)
            to_sib(cc, x, h, i)

    at_each_col(hub_reduce)

    for row in range(n_r):
        wait_recv(offr.at[row], s_off.at[row])
        for slot, t in enumerate(columns[row % 2]):
            at = pl.ds(t * supers + row // 2, rows_dev, stride=nb * supers)
            off_ref[at, :] = -offr[row, slot]

    def hub_gather(cc, other):
        h = cc // 2
        edge = 0 if cc == low else n_c - 1
        for i in range(parts):
            wait_recv(*chunk(x, 1 - h, i))
            forward(cc, x, 1 - h, i, r, edge)
            if i % 2 == 0:
                forward(cc, x, 1 - h, i, par, c)
            wait_recv(*chunk(away, h, i))
            if i % 2 == 1:
                forward(cc, away, h, i, r, other)
            to_sib(cc, x, 1 - h, i)
            to_sib(cc, away, h, i)
        for i in [*range(0, parts, 2), *range(1, parts, 2)]:
            wait_recv(*chunk(away, 1 - h, i))
            if i % 2 == 0:
                forward(cc, away, 1 - h, i, r, edge)
            to_sib(cc, away, 1 - h, i)

    def edge_gather(cc, *_):
        h = cc // 2
        for i in range(parts):
            wait_recv(*chunk(x, h, i))
            forward(cc, x, h, i, par, c)
            to_sib(cc, x, h, i)
        for i in range(parts):
            wait_recv(*chunk(x, 1 - h, i))
            if i % 2 == 1:
                forward(cc, x, 1 - h, i, par, c)
            to_sib(cc, x, 1 - h, i)
            wait_recv(*chunk(away, h, i))
            to_sib(cc, away, h, i)
        for i in range(parts):
            wait_recv(*chunk(away, 1 - h, i))
            to_sib(cc, away, 1 - h, i)

    at_each_col(hub_gather, edge_gather)
    for s in range(supers):
        for h in range(2):
            for i in range(parts):
                wait_recv(res.at[s, 1 - k, rows_at(h, i), :], s_sib.at[(s * 2 + h) * parts + i])

    wait_sends()

    @pl.when(is_hub)
    def _():
        for h in range(nb):
            copy_to(vpart.at[:, v_cols(h)], vrecv.at[:, v_cols(h)], s_v.at[h], sib, c, v_slot + h).wait_send()

    for rr in range(n_r):
        @pl.when((r == rr) & sends_d)
        def _():
            copy_to(d_src(rr, away), d_slice(rr), s_d.at[rr], par, c, 0).wait_send()

        @pl.when((r == rr) & is_hub)
        def _():
            copy_to(d_src(rr, x), d_slice(rr), s_d.at[rr], sib, c, 1).wait_send()

        @pl.when((rr == par) & is_hub)
        def _():
            copy_to(d_slice(rr), d_slice(rr), s_d.at[rr], sib, c, 2).wait_send()

        @pl.when((rr == par) & is_edge & (k == 1))
        def _():
            copy_to(d_slice(rr), d_slice(rr), s_d.at[rr], r, hub, 3).wait_send()


def unpack_kernel(supers, nb, off_in, res, off_out, diag_out, stage, sems):
    copies = [pltpu.make_async_copy(off_in, off_out, sems.at[supers * nb])]
    copies[0].start()
    place = {pair: (core, b) for core, some in enumerate(pairs_of(nb)) for b, pair in enumerate(some)}
    for s in range(supers):
        for i in range(nb):
            for j in range(nb):
                core, b = place[max(i, j), min(i, j)]
                v = res[s, core, b * LANES : (b + 1) * LANES, :]
                stage[s, i * LANES : (i + 1) * LANES, j * LANES : (j + 1) * LANES] = v if i >= j else jnp.transpose(v)
            at = (s, pl.ds(i * LANES, LANES))
            copies.append(pltpu.make_async_copy(stage.at[at], diag_out.at[at], sems.at[s * nb + i]))
            copies[-1].start()
    for cp in copies:
        cp.wait()


def fused_body(sigma_anc, anc_factor, diag_inverse, pattern):
    rows_dev, supers, width = anc_factor.shape
    n_r = lax.axis_size("row")
    n_c = lax.axis_size("col")
    total_rows = rows_dev * n_r * n_c
    nb = width // LANES
    packed = len(pairs_of(nb)[0]) * LANES
    q = packed // (2 * PARTS)
    slots = len(columns_of(nb)[0])
    f32 = lambda *shape: pltpu.VMEM(shape, jnp.float32)
    dma = lambda n: pltpu.SemaphoreType.DMA((n,))
    vm = pl.BlockSpec(memory_space=pltpu.VMEM)
    linear = jnp.transpose(anc_factor.reshape(rows_dev, supers, nb, LANES), (0, 2, 1, 3))
    linear = linear.reshape(rows_dev * nb * supers, LANES)
    hbm = pl.BlockSpec(memory_space=pl.ANY)
    off, res = pl.pallas_call(
        functools.partial(fused_kernel, n_r, n_c, supers, width, rows_dev, total_rows // pattern.shape[1], PARTS),
        out_shape=(
            pltpu.VMEM((rows_dev * supers * nb, LANES), jnp.float32),
            pltpu.VMEM((supers, 2, packed, LANES), jnp.float32),
        ),
        in_specs=[hbm, hbm, hbm, pl.BlockSpec(memory_space=pltpu.SMEM)],
        out_specs=(vm, vm),
        scratch_shapes=[
            f32(*sigma_anc.shape),
            f32(*linear.shape),
            f32(supers, rows_dev, width),
            f32(n_r * rows_dev, n_c * rows_dev),
            f32(2, n_c, rows_dev, width),
            f32(2, n_c, 2 * rows_dev, n_c * rows_dev),
            f32(width, width),
            f32(n_r, 2 * rows_dev, width),
            f32(2 * n_r * rows_dev, width),
            f32(2 * n_r * rows_dev, width),
            f32(slots, n_r, 2, rows_dev, LANES),
            f32(n_r, slots, rows_dev, LANES),
            f32(packed, LANES),
            f32(PARTS, q, LANES),
            dma(64 + 16 * PARTS),
            dma(2 * n_c), dma(2 * n_c), dma(n_r), dma(2), dma(nb), dma(n_r), dma(PARTS),
            dma(2 * supers * PARTS), dma(2 * supers * PARTS), dma(4),
        ],
        compiler_params=pltpu.CompilerParams(
            collective_id=0, has_side_effects=True, vmem_limit_bytes=58 * 1024 * 1024
        ),
    )(sigma_anc, linear, diag_inverse, pattern)
    off, diag = pl.pallas_call(
        functools.partial(unpack_kernel, supers, nb),
        out_shape=(
            jax.ShapeDtypeStruct(off.shape, jnp.float32),
            jax.ShapeDtypeStruct((supers, width, width), jnp.float32),
        ),
        in_specs=[vm, vm],
        out_specs=(hbm, hbm),
        scratch_shapes=[f32(supers, width, width), dma(supers * nb + 1)],
        compiler_params=pltpu.CompilerParams(vmem_limit_bytes=8 * 1024 * 1024),
    )(off, res)
    off = jnp.transpose(off.reshape(rows_dev, nb, supers, LANES), (0, 2, 1, 3))
    return off.reshape(anc_factor.shape), diag


def fits(sigma_anc, anc_factor, diag_inverse):
    rows_dev, supers, width = anc_factor.shape
    n_r = lax.axis_size("row")
    n_c = lax.axis_size("col")
    nb = width // LANES
    return (
        n_r == n_c
        and n_r == 2 * supers
        and supers == 2
        and sigma_anc.shape[0] == sigma_anc.shape[1]
        and diag_inverse.shape[2] % LANES == 0
        and nb % 4 == 0
        and rows_dev % SUBLANES == 0
        and width % (n_c * SUBLANES) == 0
        and len(pairs_of(nb)[0]) == len(pairs_of(nb)[1])
        and (len(pairs_of(nb)[0]) * LANES) % (2 * PARTS * SUBLANES) == 0
    )


def plain_body(sigma_anc, anc_factor, diag_inverse, pattern):
    precise = lax.Precision.HIGHEST
    rows_dev, supers, super_width = anc_factor.shape
    row_count = lax.axis_size("row")
    col_count = lax.axis_size("col")
    position = lax.axis_index("row") * col_count + lax.axis_index("col")
    total_rows = rows_dev * row_count * col_count
    block_size = total_rows // pattern.shape[1]
    flat_mask = jnp.repeat(pattern.astype(jnp.float32), block_size, axis=1)
    own_mask = jnp.transpose(lax.dynamic_slice_in_dim(flat_mask, position * rows_dev, rows_dev, 1))[
        :, :, None
    ]
    device_total = row_count * col_count
    share = -(-super_width // device_total)
    masked_factor = anc_factor * own_mask
    flattened = masked_factor.reshape(rows_dev, -1)
    gathered = lax.all_gather(flattened, "row", axis=0, tiled=True)
    stacked = gathered.reshape(row_count, rows_dev, flattened.shape[1])
    turned = lax.all_to_all(stacked, "col", split_axis=0, concat_axis=1, tiled=True)
    column_block = turned.reshape(row_count * rows_dev, flattened.shape[1])
    summed_rows = lax.psum_scatter(
        jnp.dot(sigma_anc, column_block, precision=precise, preferred_element_type=jnp.float32),
        "col",
        scatter_dimension=0,
        tiled=True,
    )
    off_factor = -(summed_rows.reshape(masked_factor.shape) * own_mask)
    both_rows = jnp.concatenate([masked_factor, off_factor], axis=0)
    column_piece = lax.all_gather(diag_inverse, "row", axis=2, tiled=True)
    product = jnp.einsum("rsk,skj->rsj", both_rows, column_piece, precision=precise)
    own_rows = lax.dynamic_slice_in_dim(column_piece, position * share, share, 1)
    scaled = product[:rows_dev]
    sel_off = product[rows_dev:]
    diag_term = jnp.einsum("skj,skl->sjl", own_rows, own_rows, precision=precise)
    partial_value = diag_term - jnp.einsum("rsj,rsl->sjl", scaled, sel_off, precision=precise)
    sel_diag = lax.psum(partial_value, ("row", "col"))
    return (sel_off, sel_diag)


def body(sigma_anc, anc_factor, diag_inverse, pattern):
    run = fused_body if fits(sigma_anc, anc_factor, diag_inverse) else plain_body
    return run(sigma_anc, anc_factor, diag_inverse, pattern)


def solution(mesh):
    return jax.shard_map(
        body,
        mesh=mesh,
        in_specs=(
            P(("grp", "row"), "col"),
            P(("grp", "row", "col"), None, None),
            P("grp", None, "row"),
            P(),
        ),
        out_specs=(P(("grp", "row", "col"), None, None), P("grp", None, None)),
        check_vma=False,
    )
```

```python
import functools
import math

import jax
import jax.numpy as jnp
from jax import lax
from jax.experimental import pallas as pl
from jax.experimental.pallas import tpu as pltpu
from jax.sharding import PartitionSpec as P

LANES = 128
SUBLANES = 8
PARTS = 4


def split(x):
    high = x.astype(jnp.bfloat16)
    low = (x - high.astype(jnp.float32)).astype(jnp.bfloat16)
    return high, low


def dot3(a, b, contract=((1,), (0,))):
    (ah, al), (bh, bl) = a, b
    f = lambda u, v: lax.dot_general(u, v, (contract, ((), ())), preferred_element_type=jnp.float32)
    return f(ah, bh) + (f(ah, bl) + f(al, bh))


def columns_of(nb):
    return [[j for j in range(nb) if (j + j // 2) % 2 == core] for core in range(2)]


def pairs_of(nb):
    columns = columns_of(nb)
    pairs = [[], []]
    every = [(i, j) for i in range(nb) for j in range(i + 1)]
    owners = lambda pair: [core for core in range(2) if pair[0] in columns[core] or pair[1] in columns[core]]
    for pair in sorted(every, key=lambda p: len(owners(p))):
        pairs[min(owners(pair), key=lambda core: len(pairs[core]))].append(pair)
    return pairs


def fused_kernel(
    n_r, n_c, supers, width, rows_dev, block_size, parts,
    sig_hbm, a_hbm, d_ref, pat_hbm,
    off_out, res,
    pat_ref, sig_ref, a_ref, av, sig_t, wz, sq, dfull, scl, vpart, vrecv, of, offr, gpart, grecv, mine, off_ref, spare,
    send_sems, s_w, s_sq, s_d, s_scl, s_v, s_off, s_h, s_g, s_sib, s_mine, local_sems,
):
    r = lax.axis_index("row")
    c = lax.axis_index("col")
    x = r // 2
    k = r % 2
    away = 1 - x
    sib = 2 * x + 1 - k
    par = 2 * away + k
    dia = 2 * away + 1 - k
    piece = width // n_r
    nb = width // LANES
    block_rows = rows_dev * n_c
    side_rows = 2 * rows_dev
    columns = columns_of(nb)
    pairs = pairs_of(nb)
    q = len(pairs[0]) * LANES // (2 * parts)
    low = n_c // 2 - 1
    side = c // 2
    mate = 4 * side + 1 - c
    hub = low + side
    is_hub = hub == c
    is_edge = hub != c
    single = [[] for _ in range(n_c)]
    bulk = [[0, 0] for _ in range(n_c)]
    late = [0]
    bulk_slot, v_slot, single_slot = 4, 6, 7

    def copy_to(src, dst, rsem, row, col, slot):
        return pltpu.make_async_remote_copy(
            src_ref=src, dst_ref=dst, send_sem=send_sems.at[slot], recv_sem=rsem,
            device_id={"row": row, "col": col}, device_id_type=pl.DeviceIdType.MESH,
        )

    def at_each_col(hub_part, edge_part=None):
        for cc in range(n_c):
            hub_col = low + cc // 2
            part = hub_part if cc == hub_col else edge_part
            if part is not None:
                pl.when(c == cc)(functools.partial(part, cc, n_c - 1 - cc))

    def post(cc, refs, row, col):
        bulk[cc][late[0]] += math.prod(refs()[0].shape)
        copy_to(*refs(), row, col, bulk_slot + late[0]).start()

    def post_single(cc, refs, row, col):
        slot = single_slot + len(single[cc])
        make = lambda: copy_to(*refs(), row, col, slot)
        make().start()
        single[cc].append(make)

    def wait_sends(part):
        def at(cc, *_):
            whole = spare.at[pl.ds(0, bulk[cc][part] // LANES), :]
            pltpu.make_async_copy(whole, whole, send_sems.at[bulk_slot + part]).wait()
            if part == 0:
                for make in single[cc]:
                    make().wait_send()

        at_each_col(at, at)

    def wait_recv(dst, rsem):
        pltpu.make_async_copy(dst, dst, rsem).wait()

    loads = [
        pltpu.make_async_copy(a_hbm, a_ref, local_sems.at[2]),
        pltpu.make_async_copy(sig_hbm, sig_ref, local_sems.at[3]),
        pltpu.make_async_copy(pat_hbm, pat_ref, local_sems.at[1]),
    ]
    for cp in loads:
        cp.start()
    barrier = pltpu.get_barrier_semaphore()
    sig = lambda row, col: pl.semaphore_signal(
        barrier, inc=1, device_id={"row": row, "col": col}, device_id_type=pl.DeviceIdType.MESH
    )
    for dc in range(1, n_c):
        sig(r, (c + dc) % n_c)
    for row in (sib, par, dia):
        sig(row, c)
        sig(row, mate)

    def mask_of(first, rows, s):
        row = first + lax.broadcasted_iota(jnp.int32, (rows, 1), 0)
        m = jnp.zeros((rows, 1), jnp.float32)
        for b in range(pat_ref.shape[1]):
            inside = (row >= b * block_size) & (row < (b + 1) * block_size)
            m = jnp.where(inside, pat_ref[s, b].astype(jnp.float32), m)
        return m

    loads[2].wait()
    loads[0].wait()
    for s in range(supers):
        mask = mask_of((r * n_c + c) * rows_dev, rows_dev, s)
        for t in range(nb):
            rows = a_ref[pl.ds(t * supers + s, rows_dev, stride=nb * supers), :]
            av[s, :, t * LANES : (t + 1) * LANES] = rows * mask
    loads[1].wait()
    sig_t[...] = jnp.transpose(sig_ref[...])

    pl.semaphore_wait(barrier, n_c + 5)

    rows_w = lambda own, j: (wz.at[own, j], s_w.at[own * n_c + j])
    rows_s = lambda own, j: (sq.at[own, j], s_sq.at[n_c if own else j])
    half_of = lambda h: sig_t.at[pl.ds(h * side_rows, side_rows), :]
    d_slice = lambda rr: dfull.at[pl.ds(rr * piece, width - rr * piece), pl.ds(rr * piece, piece)]
    d_src = lambda rr, s: d_ref.at[s, pl.ds(rr * piece, width - rr * piece), :]
    sends_d = (is_hub & (k == 0)) | (is_edge & (k == 1))

    def hub_first(cc, other):
        post(cc, lambda: (av.at[away], *rows_w(1, cc)), par, c)
        post_single(cc, lambda: (half_of(1 - cc // 2), *rows_s(0, cc)), r, other)
        post(cc, lambda: (av.at[x], *rows_w(0, cc)), r, other)
        post_single(cc, lambda: (half_of(cc // 2), *rows_s(1, cc)), par, c)

    def edge_first(cc, other):
        near = low + cc // 2
        post(cc, lambda: (av.at[away], *rows_w(1, cc)), par, c)
        post(cc, lambda: (av.at[x], *rows_w(0, cc)), r, near)
        post_single(cc, lambda: (half_of(1 - cc // 2), *rows_s(0, cc)), r, n_c - 1 - near)
        post_single(cc, lambda: (half_of(cc // 2), *rows_s(0, cc)), r, near)

    at_each_col(hub_first, edge_first)
    for rr in range(n_r):
        @pl.when((r == rr) & sends_d)
        def _():
            copy_to(d_src(rr, away), d_slice(rr), s_d.at[rr], par, c, 0).start()

        @pl.when((r == rr) & is_hub)
        def _():
            copy_to(d_src(rr, x), d_slice(rr), s_d.at[rr], sib, c, 1).start()
            pltpu.make_async_copy(d_src(rr, x), d_slice(rr), local_sems.at[0]).start()

    @pl.when(is_hub)
    def _():
        wz[0, c] = av[x]
        sq[0, c] = sig_t[pl.ds(pl.multiple_of(side * side_rows, SUBLANES), side_rows), :]
        for rr in range(1, n_r):
            dfull[0 : rr * piece, rr * piece : (rr + 1) * piece] = jnp.zeros((rr * piece, piece), jnp.float32)

    def hub_pass(cc, other):
        edge = 0 if cc == low else n_c - 1
        wait_recv(*rows_w(1, cc))
        post(cc, lambda: (wz.at[1, cc], *rows_w(1, cc)), r, other)
        wait_recv(*rows_w(0, edge))
        post(cc, lambda: (wz.at[0, edge], *rows_w(0, edge)), r, other)
        for j in (other, edge, n_c - 1 - edge):
            wait_recv(*rows_s(0, j))
            post_single(cc, lambda j=j: (sq.at[0, j], *rows_s(1, j)), par, c)

    def hub_pass_last(cc, other):
        edge = 0 if cc == low else n_c - 1
        wait_recv(*rows_w(1, edge))
        post(cc, lambda: (wz.at[1, edge], *rows_w(1, edge)), r, other)

    def edge_pass(cc, other):
        wait_recv(*rows_w(1, cc))
        post(cc, lambda: (wz.at[1, cc], *rows_w(1, cc)), r, low + cc // 2)

    at_each_col(hub_pass, edge_pass)
    for rr in range(n_r):
        @pl.when((rr == par) & is_hub)
        def _():
            @pl.when(k == 0)
            def _():
                wait_recv(d_slice(rr), s_d.at[rr])
                copy_to(d_slice(rr), d_slice(rr), s_d.at[rr], sib, c, 2).start()

        @pl.when((rr == par) & is_edge & (k == 1))
        def _():
            wait_recv(d_slice(rr), s_d.at[rr])
            copy_to(d_slice(rr), d_slice(rr), s_d.at[rr], r, hub, 3).start()
    at_each_col(hub_pass_last)
    for rr in range(n_r):
        @pl.when((rr == par) & is_hub & (k == 1))
        def _():
            wait_recv(d_slice(rr), s_d.at[rr])
            copy_to(d_slice(rr), d_slice(rr), s_d.at[rr], sib, c, 2).start()
    for rr in range(n_r):
        @pl.when(((rr == sib) | (rr == dia)) & is_hub)
        def _():
            wait_recv(d_slice(rr), s_d.at[rr])

        @pl.when((rr == r) & is_hub)
        def _():
            pltpu.make_async_copy(d_src(rr, x), d_slice(rr), local_sems.at[0]).wait()

    over_rows = ((0,), (0,))
    lanes = lambda j: slice(j * LANES, (j + 1) * LANES)
    cut = lambda pair, j: (pair[0][:, lanes(j)], pair[1][:, lanes(j)])
    mask_rows = lambda: jnp.concatenate(
        [mask_of((rr * n_c + 2 * side) * rows_dev, side_rows, x) for rr in range(n_r)], axis=0
    )

    @pl.when(is_hub)
    def _():
        own = [wz[o, pl.ds(2 * side, 2)].reshape(side_rows, width) for o in range(2)]
        near = split(jnp.concatenate(own, axis=0))
        for j in range(0, width, LANES):
            ds = split(dfull[j:, j : j + LANES])
            v = dot3((near[0][:, j:], near[1][:, j:]), ds)
            scl[r, :, j : j + LANES] = v[:side_rows]
            scl[par, :, j : j + LANES] = v[side_rows:]

    def hub_scl(cc, *_):
        post(cc, lambda: (scl.at[r], scl.at[r], s_scl.at[0]), sib, c)
        post(cc, lambda: (scl.at[par], scl.at[par], s_scl.at[0]), sib, c)

    at_each_col(hub_scl)

    @pl.when(is_hub)
    def _():
        dz = split(dfull[pl.ds(pl.multiple_of(side * (width // 2), SUBLANES), width // 2), :])
        for core in range(2):
            @pl.when(k == core)
            def _():
                for b, (i, j) in enumerate(pairs[core]):
                    gpart[lanes(b), :] = dot3(cut(dz, i), cut(dz, j), over_rows)

    def v_of(own):
        sigma = split(sq[own].reshape(n_r * side_rows, block_rows))
        return sigma, split(wz[own].reshape(block_rows, width))

    def hub_wait(own, cc, other):
        edge = 0 if cc == low else n_c - 1
        for j in (other, n_c - 1 - edge):
            wait_recv(*rows_w(own, j))
        if own == 1:
            wait_recv(sq.at[1], s_sq.at[n_c])

    at_each_col(functools.partial(hub_wait, 0))

    @pl.when(is_hub)
    def _():
        vpart[...] = dot3(*v_of(0))

    at_each_col(functools.partial(hub_wait, 1))
    v_cols = lambda h: slice(h * LANES, (h + 1) * LANES)

    @pl.when(is_hub)
    def _():
        sigma, ws = v_of(1)
        for h in range(nb):
            vpart[:, v_cols(h)] = vpart[:, v_cols(h)] + dot3(sigma, cut(ws, h))
            copy_to(vpart.at[:, v_cols(h)], vrecv.at[:, v_cols(h)], s_v.at[0], sib, c, v_slot).start()

        wait_recv(scl.at[pl.ds(0, 2)], s_scl.at[0])
        all_scl = split(scl[...].reshape(n_r * side_rows, width))
        wait_recv(vrecv, s_v.at[0])
        vs = split((vpart[...] + vrecv[...]) * mask_rows())
        for core in range(2):
            @pl.when(k == core)
            def _():
                ofs = {}
                for slot, j in enumerate(columns[core]):
                    at = j * LANES
                    v = dot3((vs[0][:, at:], vs[1][:, at:]), split(dfull[at:, at : at + LANES]))
                    of[slot] = v.reshape(n_r, 2, rows_dev, LANES)
                    ofs[j] = split(v)
                for b, (i, j) in enumerate(pairs[core]):
                    left, right = (cut(all_scl, i), ofs[j]) if j in ofs else (ofs[i], cut(all_scl, j))
                    gpart[lanes(b), :] += dot3(left, right, over_rows)

    rows_at = lambda h, i: pl.ds((h * parts + i) * q, q)
    chunk = lambda s, h, i: (res.at[s, k, rows_at(h, i), :], s_g.at[(s * 2 + h) * parts + i])
    held = lambda s, h, i: res.at[s, k, rows_at(h, i), :]

    def hub_scatter(cc, other):
        for i in range(parts):
            post(cc, lambda i=i: (gpart.at[rows_at(1 - cc // 2, i), :], grecv.at[i], s_h.at[i]), r, other)
        edge = 0 if cc == low else n_c - 1
        for row in (sib, par, dia):
            post(cc, lambda row=row: (of.at[:, row, cc - 2 * (cc // 2)], offr.at[r], s_off.at[0]), row, cc)
        for row in (r, sib, par, dia):
            post(cc, lambda row=row: (of.at[:, row, edge - 2 * (cc // 2)], offr.at[r], s_off.at[0]), row, edge)
        pltpu.make_async_copy(of.at[:, r, cc - 2 * (cc // 2)], offr.at[r], s_off.at[0]).start()

    at_each_col(hub_scatter)
    late[0] = 1

    def forward(cc, s, h, i, row, col):
        post(cc, lambda: (held(s, h, i), *chunk(s, h, i)), row, col)

    def to_sib(cc, s, h, i):
        post(cc, lambda: (held(s, h, i), held(s, h, i), s_sib.at[0]), sib, c)

    def hub_reduce(cc, other):
        h = cc // 2
        edge = 0 if cc == low else n_c - 1
        for i in range(parts):
            wait_recv(grecv.at[i], s_h.at[i])
            mine[i] = gpart[rows_at(h, i), :] + grecv[i]
            pltpu.make_async_copy(mine.at[i], held(x, h, i), s_mine.at[0]).start()
            for row, col in ((par, c), (r, other), (r, edge)):
                post(cc, lambda i=i: (mine.at[i], *chunk(x, h, i)), row, col)
            post(cc, lambda i=i: (mine.at[i], held(x, h, i), s_sib.at[0]), sib, c)

    at_each_col(hub_reduce)

    wait_recv(offr, s_off.at[0])
    for row in range(n_r):
        for slot, t in enumerate(columns[row % 2]):
            at = pl.ds(t * supers + row // 2, rows_dev, stride=nb * supers)
            off_ref[at, :] = -offr[row, slot]
    off_copy = pltpu.make_async_copy(off_ref, off_out, local_sems.at[2])
    off_copy.start()
    wait_sends(0)

    def hub_gather(cc, other):
        h = cc // 2
        edge = 0 if cc == low else n_c - 1
        for i in range(parts):
            wait_recv(*chunk(x, 1 - h, i))
            forward(cc, x, 1 - h, i, r, edge)
            if i % 2 == 0:
                forward(cc, x, 1 - h, i, par, c)
            wait_recv(*chunk(away, h, i))
            if i % 2 == 1:
                forward(cc, away, h, i, r, other)
            to_sib(cc, x, 1 - h, i)
            to_sib(cc, away, h, i)
        for i in [*range(0, parts, 2), *range(1, parts, 2)]:
            wait_recv(*chunk(away, 1 - h, i))
            if i % 2 == 0:
                forward(cc, away, 1 - h, i, r, edge)
            to_sib(cc, away, 1 - h, i)

    def edge_gather(cc, *_):
        h = cc // 2
        for i in range(parts):
            wait_recv(*chunk(x, h, i))
            forward(cc, x, h, i, par, c)
            to_sib(cc, x, h, i)
        for i in range(parts):
            wait_recv(*chunk(x, 1 - h, i))
            if i % 2 == 1:
                forward(cc, x, 1 - h, i, par, c)
            to_sib(cc, x, 1 - h, i)
            wait_recv(*chunk(away, h, i))
            to_sib(cc, away, h, i)
        for i in range(parts):
            wait_recv(*chunk(away, 1 - h, i))
            to_sib(cc, away, 1 - h, i)

    at_each_col(hub_gather, edge_gather)
    theirs = res.at[:, 1 - k]
    wait_recv(theirs, s_sib.at[0])
    @pl.when(is_hub)
    def _():
        pltpu.make_async_copy(mine, mine, s_mine.at[0]).wait()

    off_copy.wait()
    wait_sends(1)

    @pl.when(is_hub)
    def _():
        copy_to(vpart, vrecv, s_v.at[0], sib, c, v_slot).wait_send()

    for rr in range(n_r):
        @pl.when((r == rr) & sends_d)
        def _():
            copy_to(d_src(rr, away), d_slice(rr), s_d.at[rr], par, c, 0).wait_send()

        @pl.when((r == rr) & is_hub)
        def _():
            copy_to(d_src(rr, x), d_slice(rr), s_d.at[rr], sib, c, 1).wait_send()

        @pl.when((rr == par) & is_hub)
        def _():
            copy_to(d_slice(rr), d_slice(rr), s_d.at[rr], sib, c, 2).wait_send()

        @pl.when((rr == par) & is_edge & (k == 1))
        def _():
            copy_to(d_slice(rr), d_slice(rr), s_d.at[rr], r, hub, 3).wait_send()


def unpack_kernel(supers, nb, off_in, res, off_out, diag_out, stage, sems):
    copies = [pltpu.make_async_copy(off_in, off_out, sems.at[supers * nb])]
    copies[0].start()
    place = {pair: (core, b) for core, some in enumerate(pairs_of(nb)) for b, pair in enumerate(some)}
    for s in range(supers):
        for i in range(nb):
            for j in range(nb):
                core, b = place[max(i, j), min(i, j)]
                v = res[s, core, b * LANES : (b + 1) * LANES, :]
                stage[s, i * LANES : (i + 1) * LANES, j * LANES : (j + 1) * LANES] = v if i >= j else jnp.transpose(v)
            at = (s, pl.ds(i * LANES, LANES))
            copies.append(pltpu.make_async_copy(stage.at[at], diag_out.at[at], sems.at[s * nb + i]))
            copies[-1].start()
    for cp in copies:
        cp.wait()


def fused_body(sigma_anc, anc_factor, diag_inverse, pattern):
    rows_dev, supers, width = anc_factor.shape
    n_r = lax.axis_size("row")
    n_c = lax.axis_size("col")
    total_rows = rows_dev * n_r * n_c
    nb = width // LANES
    packed = len(pairs_of(nb)[0]) * LANES
    q = packed // (2 * PARTS)
    slots = len(columns_of(nb)[0])
    f32 = lambda *shape: pltpu.VMEM(shape, jnp.float32)
    dma = lambda n: pltpu.SemaphoreType.DMA((n,))
    vm = pl.BlockSpec(memory_space=pltpu.VMEM)
    linear = jnp.transpose(anc_factor.reshape(rows_dev, supers, nb, LANES), (0, 2, 1, 3))
    linear = linear.reshape(rows_dev * nb * supers, LANES)
    hbm = pl.BlockSpec(memory_space=pl.ANY)
    off, res = pl.pallas_call(
        functools.partial(fused_kernel, n_r, n_c, supers, width, rows_dev, total_rows // pattern.shape[1], PARTS),
        out_shape=(
            pltpu.VMEM((rows_dev * supers * nb, LANES), jnp.float32),
            pltpu.VMEM((supers, 2, packed, LANES), jnp.float32),
        ),
        in_specs=[hbm, hbm, hbm, hbm],
        out_specs=(hbm, hbm),
        scratch_shapes=[
            pltpu.SMEM(pattern.shape, jnp.int32),
            f32(*sigma_anc.shape),
            f32(*linear.shape),
            f32(supers, rows_dev, width),
            f32(n_r * rows_dev, n_c * rows_dev),
            f32(2, n_c, rows_dev, width),
            f32(2, n_c, 2 * rows_dev, n_c * rows_dev),
            f32(width, width),
            f32(n_r, 2 * rows_dev, width),
            f32(2 * n_r * rows_dev, width),
            f32(2 * n_r * rows_dev, width),
            f32(slots, n_r, 2, rows_dev, LANES),
            f32(n_r, slots, rows_dev, LANES),
            f32(packed, LANES),
            f32(PARTS, q, LANES),
            f32(PARTS, q, LANES),
            f32(*linear.shape),
            f32(8 * packed + 8 * n_r * rows_dev * nb, LANES),
            dma(7 + n_c + 1),
            dma(2 * n_c), dma(n_c + 1), dma(n_r), dma(1), dma(1), dma(1), dma(PARTS),
            dma(2 * supers * PARTS), dma(1), dma(1), dma(4),
        ],
        compiler_params=pltpu.CompilerParams(
            collective_id=0, has_side_effects=True, vmem_limit_bytes=58 * 1024 * 1024
        ),
    )(sigma_anc, linear, diag_inverse, pattern)
    off, diag = pl.pallas_call(
        functools.partial(unpack_kernel, supers, nb),
        out_shape=(
            jax.ShapeDtypeStruct(off.shape, jnp.float32),
            jax.ShapeDtypeStruct((supers, width, width), jnp.float32),
        ),
        in_specs=[vm, vm],
        out_specs=(hbm, hbm),
        scratch_shapes=[f32(supers, width, width), dma(supers * nb + 1)],
        compiler_params=pltpu.CompilerParams(vmem_limit_bytes=8 * 1024 * 1024),
    )(off, res)
    off = jnp.transpose(off.reshape(rows_dev, nb, supers, LANES), (0, 2, 1, 3))
    return off.reshape(anc_factor.shape), diag


def fits(sigma_anc, anc_factor, diag_inverse):
    rows_dev, supers, width = anc_factor.shape
    n_r = lax.axis_size("row")
    n_c = lax.axis_size("col")
    nb = width // LANES
    return (
        n_r == n_c
        and n_r == 2 * supers
        and supers == 2
        and sigma_anc.shape[0] == sigma_anc.shape[1]
        and diag_inverse.shape[2] % LANES == 0
        and nb % 4 == 0
        and rows_dev % SUBLANES == 0
        and width % (n_c * SUBLANES) == 0
        and len(pairs_of(nb)[0]) == len(pairs_of(nb)[1])
        and (len(pairs_of(nb)[0]) * LANES) % (2 * PARTS * SUBLANES) == 0
    )


def plain_body(sigma_anc, anc_factor, diag_inverse, pattern):
    precise = lax.Precision.HIGHEST
    rows_dev, supers, super_width = anc_factor.shape
    row_count = lax.axis_size("row")
    col_count = lax.axis_size("col")
    position = lax.axis_index("row") * col_count + lax.axis_index("col")
    total_rows = rows_dev * row_count * col_count
    block_size = total_rows // pattern.shape[1]
    flat_mask = jnp.repeat(pattern.astype(jnp.float32), block_size, axis=1)
    own_mask = jnp.transpose(lax.dynamic_slice_in_dim(flat_mask, position * rows_dev, rows_dev, 1))[
        :, :, None
    ]
    device_total = row_count * col_count
    share = -(-super_width // device_total)
    masked_factor = anc_factor * own_mask
    flattened = masked_factor.reshape(rows_dev, -1)
    gathered = lax.all_gather(flattened, "row", axis=0, tiled=True)
    stacked = gathered.reshape(row_count, rows_dev, flattened.shape[1])
    turned = lax.all_to_all(stacked, "col", split_axis=0, concat_axis=1, tiled=True)
    column_block = turned.reshape(row_count * rows_dev, flattened.shape[1])
    summed_rows = lax.psum_scatter(
        jnp.dot(sigma_anc, column_block, precision=precise, preferred_element_type=jnp.float32),
        "col",
        scatter_dimension=0,
        tiled=True,
    )
    off_factor = -(summed_rows.reshape(masked_factor.shape) * own_mask)
    both_rows = jnp.concatenate([masked_factor, off_factor], axis=0)
    column_piece = lax.all_gather(diag_inverse, "row", axis=2, tiled=True)
    product = jnp.einsum("rsk,skj->rsj", both_rows, column_piece, precision=precise)
    own_rows = lax.dynamic_slice_in_dim(column_piece, position * share, share, 1)
    scaled = product[:rows_dev]
    sel_off = product[rows_dev:]
    diag_term = jnp.einsum("skj,skl->sjl", own_rows, own_rows, precision=precise)
    partial_value = diag_term - jnp.einsum("rsj,rsl->sjl", scaled, sel_off, precision=precise)
    sel_diag = lax.psum(partial_value, ("row", "col"))
    return (sel_off, sel_diag)


def body(sigma_anc, anc_factor, diag_inverse, pattern):
    run = fused_body if fits(sigma_anc, anc_factor, diag_inverse) else plain_body
    return run(sigma_anc, anc_factor, diag_inverse, pattern)


def solution(mesh):
    return jax.shard_map(
        body,
        mesh=mesh,
        in_specs=(
            P(("grp", "row"), "col"),
            P(("grp", "row", "col"), None, None),
            P("grp", None, "row"),
            P(),
        ),
        out_specs=(P(("grp", "row", "col"), None, None), P("grp", None, None)),
        check_vma=False,
    )
```

```python
import functools
import math

import jax
import jax.numpy as jnp
from jax import lax
from jax.experimental import pallas as pl
from jax.experimental.pallas import tpu as pltpu
from jax.sharding import PartitionSpec as P

LANES = 128
SUBLANES = 8
PARTS = 4


def split(x):
    high = x.astype(jnp.bfloat16)
    low = (x - high.astype(jnp.float32)).astype(jnp.bfloat16)
    return high, low


def dot3(a, b, contract=((1,), (0,))):
    (ah, al), (bh, bl) = a, b
    f = lambda u, v: lax.dot_general(u, v, (contract, ((), ())), preferred_element_type=jnp.float32)
    return f(ah, bh) + (f(ah, bl) + f(al, bh))


def columns_of(nb):
    return [[j for j in range(nb) if (j + j // 2) % 2 == core] for core in range(2)]


def pairs_of(nb):
    columns = columns_of(nb)
    pairs = [[], []]
    every = [(i, j) for i in range(nb) for j in range(i + 1)]
    owners = lambda pair: [core for core in range(2) if pair[0] in columns[core] or pair[1] in columns[core]]
    for pair in sorted(every, key=lambda p: len(owners(p))):
        pairs[min(owners(pair), key=lambda core: len(pairs[core]))].append(pair)
    return pairs


def fused_kernel(
    n_r, n_c, supers, width, rows_dev, block_size, parts,
    sig_hbm, a_hbm, d_ref, pat_hbm,
    off_out, res,
    pat_ref, sig_ref, a_ref, av, sig_t, wz, sq, dfull, scl, vpart, vrecv, of, offr, gpart, grecv, mine, off_ref, spare,
    send_sems, s_w, s_sq, s_d, s_scl, s_v, s_off, s_h, s_g, s_sib, s_mine, local_sems,
):
    r = lax.axis_index("row")
    c = lax.axis_index("col")
    x = r // 2
    k = r % 2
    away = 1 - x
    sib = 2 * x + 1 - k
    par = 2 * away + k
    dia = 2 * away + 1 - k
    piece = width // n_r
    nb = width // LANES
    block_rows = rows_dev * n_c
    side_rows = 2 * rows_dev
    columns = columns_of(nb)
    pairs = pairs_of(nb)
    q = len(pairs[0]) * LANES // (2 * parts)
    low = n_c // 2 - 1
    side = c // 2
    mate = 4 * side + 1 - c
    hub = low + side
    is_hub = hub == c
    is_edge = hub != c
    single = [[] for _ in range(n_c)]
    bulk = [[0, 0] for _ in range(n_c)]
    late = [0]
    direct = parts // 2
    bulk_slot, v_slot, single_slot = 4, 6, 7

    def copy_to(src, dst, rsem, row, col, slot):
        return pltpu.make_async_remote_copy(
            src_ref=src, dst_ref=dst, send_sem=send_sems.at[slot], recv_sem=rsem,
            device_id={"row": row, "col": col}, device_id_type=pl.DeviceIdType.MESH,
        )

    def at_each_col(hub_part, edge_part=None):
        for cc in range(n_c):
            hub_col = low + cc // 2
            part = hub_part if cc == hub_col else edge_part
            if part is not None:
                pl.when(c == cc)(functools.partial(part, cc, n_c - 1 - cc))

    def post(cc, refs, row, col):
        bulk[cc][late[0]] += math.prod(refs()[0].shape)
        copy_to(*refs(), row, col, bulk_slot + late[0]).start()

    def post_hub(core, refs, row, col):
        if core == 0:
            for cc in (low, low + 1):
                bulk[cc][late[0]] += math.prod(refs()[0].shape)
        copy_to(*refs(), row, col, bulk_slot + late[0]).start()

    def off_refs(row, col, kind):
        return lambda: (of.at[:, row, col - 2 * side], offr.at[r], s_off.at[kind])

    def post_single(cc, refs, row, col):
        slot = single_slot + len(single[cc])
        make = lambda: copy_to(*refs(), row, col, slot)
        make().start()
        single[cc].append(make)

    def wait_sends(part):
        def at(cc, *_):
            whole = spare.at[pl.ds(0, bulk[cc][part] // LANES), :]
            pltpu.make_async_copy(whole, whole, send_sems.at[bulk_slot + part]).wait()
            if part == 0:
                for make in single[cc]:
                    make().wait_send()

        at_each_col(at, at)

    def wait_recv(dst, rsem):
        pltpu.make_async_copy(dst, dst, rsem).wait()

    loads = [
        pltpu.make_async_copy(a_hbm, a_ref, local_sems.at[2]),
        pltpu.make_async_copy(sig_hbm, sig_ref, local_sems.at[3]),
        pltpu.make_async_copy(pat_hbm, pat_ref, local_sems.at[1]),
    ]
    for cp in loads:
        cp.start()
    barrier = pltpu.get_barrier_semaphore()
    sig = lambda row, col: pl.semaphore_signal(
        barrier, inc=1, device_id={"row": row, "col": col}, device_id_type=pl.DeviceIdType.MESH
    )
    for dc in range(1, n_c):
        sig(r, (c + dc) % n_c)
    for row in (sib, par, dia):
        sig(row, c)
        sig(row, mate)

    def mask_of(first, rows, s):
        row = first + lax.broadcasted_iota(jnp.int32, (rows, 1), 0)
        m = jnp.zeros((rows, 1), jnp.float32)
        for b in range(pat_ref.shape[1]):
            inside = (row >= b * block_size) & (row < (b + 1) * block_size)
            m = jnp.where(inside, pat_ref[s, b].astype(jnp.float32), m)
        return m

    loads[2].wait()
    loads[0].wait()
    for s in range(supers):
        mask = mask_of((r * n_c + c) * rows_dev, rows_dev, s)
        for t in range(nb):
            rows = a_ref[pl.ds(t * supers + s, rows_dev, stride=nb * supers), :]
            av[s, :, t * LANES : (t + 1) * LANES] = rows * mask
    loads[1].wait()
    sig_t[...] = jnp.transpose(sig_ref[...])

    pl.semaphore_wait(barrier, n_c + 5)

    rows_w = lambda own, j: (wz.at[own, j], s_w.at[own * n_c + j])
    rows_s = lambda own, j: (sq.at[own, j], s_sq.at[n_c if own else j])
    half_rows = rows_dev // 2
    rows_h = lambda j, i: (wz.at[1, j, pl.ds(i * half_rows, half_rows), :], s_w.at[(1 + i) * n_c + j])
    half_of = lambda h: sig_t.at[pl.ds(h * side_rows, side_rows), :]
    d_slice = lambda rr: dfull.at[pl.ds(rr * piece, width - rr * piece), pl.ds(rr * piece, piece)]
    d_src = lambda rr, s: d_ref.at[s, pl.ds(rr * piece, width - rr * piece), :]
    sends_d = (is_hub & (k == 0)) | (is_edge & (k == 1))

    def hub_first(cc, other):
        post(cc, lambda: (av.at[away], *rows_w(1, cc)), par, c)
        post_single(cc, lambda: (half_of(1 - cc // 2), *rows_s(0, cc)), r, other)
        post(cc, lambda: (av.at[x], *rows_w(0, cc)), r, other)
        post_single(cc, lambda: (half_of(cc // 2), *rows_s(1, cc)), par, c)

    def edge_first(cc, other):
        near = low + cc // 2
        post(cc, lambda: (av.at[away], *rows_w(1, cc)), par, c)
        post(cc, lambda: (av.at[x], *rows_w(0, cc)), r, near)
        post_single(cc, lambda: (half_of(1 - cc // 2), *rows_s(0, cc)), r, n_c - 1 - near)

    at_each_col(hub_first, edge_first)
    for rr in range(n_r):
        @pl.when((r == rr) & sends_d)
        def _():
            copy_to(d_src(rr, away), d_slice(rr), s_d.at[rr], par, c, 0).start()

        @pl.when((r == rr) & is_hub)
        def _():
            copy_to(d_src(rr, x), d_slice(rr), s_d.at[rr], sib, c, 1).start()
            pltpu.make_async_copy(d_src(rr, x), d_slice(rr), local_sems.at[0]).start()

    @pl.when(is_hub)
    def _():
        wz[0, c] = av[x]
        sq[0, c] = sig_t[pl.ds(pl.multiple_of(side * side_rows, SUBLANES), side_rows), :]
        for rr in range(1, n_r):
            dfull[0 : rr * piece, rr * piece : (rr + 1) * piece] = jnp.zeros((rr * piece, piece), jnp.float32)

    def hub_pass(cc, other):
        edge = 0 if cc == low else n_c - 1
        wait_recv(*rows_w(1, cc))
        post(cc, lambda: (wz.at[1, cc], *rows_w(1, cc)), r, other)
        wait_recv(*rows_w(0, edge))
        post(cc, lambda: (wz.at[0, edge], *rows_w(0, edge)), r, other)
        for j in (other, n_c - 1 - edge):
            wait_recv(*rows_s(0, j))
            post_single(cc, lambda j=j: (sq.at[0, j], *rows_s(1, j)), par, c)

    def hub_pass_last(cc, other):
        edge = 0 if cc == low else n_c - 1
        for i in range(2):
            wait_recv(*rows_h(edge, i))
            post(cc, lambda i=i: (rows_h(edge, i)[0], *rows_h(edge, i)), r, other)
        wait_recv(*rows_s(0, edge))
        post_single(cc, lambda: (sq.at[0, edge], *rows_s(1, edge)), par, c)

    def edge_pass(cc, other):
        wait_recv(*rows_w(1, cc))
        for i in range(2):
            post(cc, lambda i=i: (rows_h(cc, i)[0], *rows_h(cc, i)), r, low + cc // 2)
        post_single(cc, lambda: (half_of(cc // 2), *rows_s(0, cc)), r, low + cc // 2)

    at_each_col(hub_pass, edge_pass)
    at_each_col(hub_pass_last)
    for rr in range(n_r):
        @pl.when((rr == par) & is_hub)
        def _():
            @pl.when(k == 0)
            def _():
                wait_recv(d_slice(rr), s_d.at[rr])
                copy_to(d_slice(rr), d_slice(rr), s_d.at[rr], sib, c, 2).start()

        @pl.when((rr == par) & is_edge & (k == 1))
        def _():
            wait_recv(d_slice(rr), s_d.at[rr])
            copy_to(d_slice(rr), d_slice(rr), s_d.at[rr], r, hub, 3).start()
    for rr in range(n_r):
        @pl.when((rr == par) & is_hub & (k == 1))
        def _():
            wait_recv(d_slice(rr), s_d.at[rr])
            copy_to(d_slice(rr), d_slice(rr), s_d.at[rr], sib, c, 2).start()
    def v_of(own):
        sigma = split(sq[own].reshape(n_r * side_rows, block_rows))
        return sigma, split(wz[own].reshape(block_rows, width))

    def hub_wait(own, cc, other):
        edge = 0 if cc == low else n_c - 1
        wait_recv(*rows_w(own, other))
        for i in range(2):
            if own == 1:
                wait_recv(*rows_h(n_c - 1 - edge, i))
            elif i == 0:
                wait_recv(*rows_w(0, n_c - 1 - edge))
        if own == 1:
            wait_recv(sq.at[1], s_sq.at[n_c])

    at_each_col(functools.partial(hub_wait, 0))

    @pl.when(is_hub)
    def _():
        vpart[...] = dot3(*v_of(0))

    for rr in range(n_r):
        @pl.when(((rr == sib) | (rr == dia)) & is_hub)
        def _():
            wait_recv(d_slice(rr), s_d.at[rr])

        @pl.when((rr == r) & is_hub)
        def _():
            pltpu.make_async_copy(d_src(rr, x), d_slice(rr), local_sems.at[0]).wait()

    rows_at = lambda h, i: pl.ds((h * parts + i) * q, q)
    over_rows = ((0,), (0,))
    lanes = lambda j: slice(j * LANES, (j + 1) * LANES)
    cut = lambda pair, j: (pair[0][:, lanes(j)], pair[1][:, lanes(j)])
    mask_rows = lambda: jnp.concatenate(
        [mask_of((rr * n_c + 2 * side) * rows_dev, side_rows, x) for rr in range(n_r)], axis=0
    )

    @pl.when(is_hub)
    def _():
        own = [wz[o, pl.ds(2 * side, 2)].reshape(side_rows, width) for o in range(2)]
        near = split(jnp.concatenate(own, axis=0))
        for j in range(0, width, LANES):
            ds = split(dfull[j:, j : j + LANES])
            v = dot3((near[0][:, j:], near[1][:, j:]), ds)
            scl[r, :, j : j + LANES] = v[:side_rows]
            scl[par, :, j : j + LANES] = v[side_rows:]

    def hub_scl(cc, *_):
        post(cc, lambda: (scl.at[r], scl.at[r], s_scl.at[0]), sib, c)
        post(cc, lambda: (scl.at[par], scl.at[par], s_scl.at[0]), sib, c)

    at_each_col(hub_scl)

    @pl.when(is_hub)
    def _():
        dz = split(dfull[pl.ds(pl.multiple_of(side * (width // 2), SUBLANES), width // 2), :])
        for core in range(2):
            @pl.when(k == core)
            def _():
                for b, (i, j) in enumerate(pairs[core]):
                    gpart[lanes(b), :] = dot3(cut(dz, i), cut(dz, j), over_rows)

    at_each_col(functools.partial(hub_wait, 1))
    far = n_c - 1 - c

    def sum_pairs(core, own_side, all_scl, ofs):
        first = (1 - own_side) * parts * q
        order = sorted(range(len(pairs[core])), key=lambda b: ((b + 1) * LANES <= first, b))
        left_parts = list(range(parts))
        ready = set()
        for b in order:
            i, j = pairs[core][b]
            left, right = (cut(all_scl, i), ofs[j]) if j in ofs else (ofs[i], cut(all_scl, j))
            gpart[lanes(b), :] += dot3(left, right, over_rows)
            ready.add(b)
            for part in list(left_parts):
                at = first + part * q
                if set(range(at // LANES, (at + q - 1) // LANES + 1)) <= ready:
                    left_parts.remove(part)
                    refs = lambda part=part: (gpart.at[rows_at(1 - own_side, part), :], grecv.at[part], s_h.at[part])
                    if core == 0:
                        bulk[low + own_side][0] += math.prod(refs()[0].shape)
                    copy_to(*refs(), r, far, bulk_slot).start()

    v_cols = lambda h: slice(h * LANES, (h + 1) * LANES)

    @pl.when(is_hub)
    def _():
        sigma, ws = v_of(1)
        for h in range(nb):
            vpart[:, v_cols(h)] = vpart[:, v_cols(h)] + dot3(sigma, cut(ws, h))
            copy_to(vpart.at[:, v_cols(h)], vrecv.at[:, v_cols(h)], s_v.at[0], sib, c, v_slot).start()

        wait_recv(scl.at[pl.ds(0, 2)], s_scl.at[0])
        all_scl = split(scl[...].reshape(n_r * side_rows, width))
        wait_recv(vrecv, s_v.at[0])
        vs = split((vpart[...] + vrecv[...]) * mask_rows())
        for core in range(2):
            @pl.when(k == core)
            def _():
                ofs = {}
                for slot, j in enumerate(columns[core]):
                    at = j * LANES
                    v = dot3((vs[0][:, at:], vs[1][:, at:]), split(dfull[at:, at : at + LANES]))
                    of[slot] = v.reshape(n_r, 2, rows_dev, LANES)
                    ofs[j] = split(v)
                for row, col, kind in ((par, c, 1), (dia, c, 1), (r, mate, 0), (sib, mate, 0), (sib, c, 0), (par, mate, 1), (dia, mate, 1)):
                    post_hub(core, off_refs(row, c if col is c else mate, kind), row, col)
                pltpu.make_async_copy(*off_refs(r, c, 0)()).start()
                for own_side in range(2):
                    pl.when(side == own_side)(functools.partial(sum_pairs, core, own_side, all_scl, ofs))

    chunk = lambda s, h, i: (res.at[s, k, rows_at(h, i), :], s_g.at[(s * 2 + h) * parts + i])
    held = lambda s, h, i: res.at[s, k, rows_at(h, i), :]

    late[0] = 1

    def forward(cc, s, h, i, row, col):
        post(cc, lambda: (held(s, h, i), *chunk(s, h, i)), row, col)

    def to_sib(cc, s, h, i):
        post(cc, lambda: (held(s, h, i), held(s, h, i), s_sib.at[0]), sib, c)

    def hub_reduce(cc, other):
        h = cc // 2
        edge = 0 if cc == low else n_c - 1
        for i in range(parts):
            wait_recv(grecv.at[i], s_h.at[i])
            mine[i] = gpart[rows_at(h, i), :] + grecv[i]
            pltpu.make_async_copy(mine.at[i], held(x, h, i), s_mine.at[0]).start()
            for row, col in ((par, c), (r, other), (r, edge)):
                post(cc, lambda i=i: (mine.at[i], *chunk(x, h, i)), row, col)
            post(cc, lambda i=i: (mine.at[i], held(x, h, i), s_sib.at[0]), sib, c)

    at_each_col(hub_reduce)

    def put_off(own):
        first = x if own else away
        wait_recv(offr.at[pl.ds(2 * first, 2)], s_off.at[0 if own else 1])
        for s in range(supers):
            @pl.when(first == s)
            def _():
                for row in (2 * s, 2 * s + 1):
                    for slot, t in enumerate(columns[row % 2]):
                        at = pl.ds(t * supers + s, rows_dev, stride=nb * supers)
                        off_ref[at, :] = -offr[row, slot]

    off_copy = lambda: pltpu.make_async_copy(off_ref, off_out, local_sems.at[2])
    put_off(True)

    @pl.when(is_hub)
    def _():
        put_off(False)
        off_copy().start()

    wait_sends(0)

    def hub_gather(cc, other):
        h = cc // 2
        edge = 0 if cc == low else n_c - 1
        for i in range(parts):
            wait_recv(*chunk(x, 1 - h, i))
            forward(cc, x, 1 - h, i, r, edge)
            forward(cc, x, 1 - h, i, par, c)
            wait_recv(*chunk(away, h, i))
            to_sib(cc, x, 1 - h, i)
            to_sib(cc, away, h, i)
        for i in range(direct, parts):
            forward(cc, away, h, i, r, n_c - 1 - edge)
        for i in range(parts):
            wait_recv(*chunk(away, 1 - h, i))
            to_sib(cc, away, 1 - h, i)

    def edge_gather(cc, *_):
        h = cc // 2
        for i in range(parts):
            wait_recv(*chunk(x, h, i))
            forward(cc, x, h, i, par, c)
            to_sib(cc, x, h, i)
        put_off(False)
        off_copy().start()
        for i in range(direct):
            wait_recv(*chunk(x, 1 - h, i))
            forward(cc, x, 1 - h, i, par, c)
            to_sib(cc, x, 1 - h, i)
        order = [(away, h, i) for i in range(parts)]
        for i in range(direct):
            order += [(away, 1 - h, i + direct), (away, 1 - h, i)]
        for i in range(direct, parts):
            order.insert(len(order) - (parts - 1 - i), (x, 1 - h, i))
        for s, g, i in order:
            wait_recv(*chunk(s, g, i))
            to_sib(cc, s, g, i)

    at_each_col(hub_gather, edge_gather)
    theirs = res.at[:, 1 - k]
    wait_recv(theirs, s_sib.at[0])
    @pl.when(is_hub)
    def _():
        pltpu.make_async_copy(mine, mine, s_mine.at[0]).wait()

    off_copy().wait()
    wait_sends(1)

    @pl.when(is_hub)
    def _():
        copy_to(vpart, vrecv, s_v.at[0], sib, c, v_slot).wait_send()

    for rr in range(n_r):
        @pl.when((r == rr) & sends_d)
        def _():
            copy_to(d_src(rr, away), d_slice(rr), s_d.at[rr], par, c, 0).wait_send()

        @pl.when((r == rr) & is_hub)
        def _():
            copy_to(d_src(rr, x), d_slice(rr), s_d.at[rr], sib, c, 1).wait_send()

        @pl.when((rr == par) & is_hub)
        def _():
            copy_to(d_slice(rr), d_slice(rr), s_d.at[rr], sib, c, 2).wait_send()

        @pl.when((rr == par) & is_edge & (k == 1))
        def _():
            copy_to(d_slice(rr), d_slice(rr), s_d.at[rr], r, hub, 3).wait_send()


def unpack_kernel(supers, nb, off_in, res, off_out, diag_out, stage, sems):
    copies = [pltpu.make_async_copy(off_in, off_out, sems.at[supers * nb])]
    copies[0].start()
    place = {pair: (core, b) for core, some in enumerate(pairs_of(nb)) for b, pair in enumerate(some)}
    for s in range(supers):
        for i in range(nb):
            for j in range(nb):
                core, b = place[max(i, j), min(i, j)]
                v = res[s, core, b * LANES : (b + 1) * LANES, :]
                stage[s, i * LANES : (i + 1) * LANES, j * LANES : (j + 1) * LANES] = v if i >= j else jnp.transpose(v)
            at = (s, pl.ds(i * LANES, LANES))
            copies.append(pltpu.make_async_copy(stage.at[at], diag_out.at[at], sems.at[s * nb + i]))
            copies[-1].start()
    for cp in copies:
        cp.wait()


def fused_body(sigma_anc, anc_factor, diag_inverse, pattern):
    rows_dev, supers, width = anc_factor.shape
    n_r = lax.axis_size("row")
    n_c = lax.axis_size("col")
    total_rows = rows_dev * n_r * n_c
    nb = width // LANES
    packed = len(pairs_of(nb)[0]) * LANES
    q = packed // (2 * PARTS)
    slots = len(columns_of(nb)[0])
    f32 = lambda *shape: pltpu.VMEM(shape, jnp.float32)
    dma = lambda n: pltpu.SemaphoreType.DMA((n,))
    vm = pl.BlockSpec(memory_space=pltpu.VMEM)
    linear = jnp.transpose(anc_factor.reshape(rows_dev, supers, nb, LANES), (0, 2, 1, 3))
    linear = linear.reshape(rows_dev * nb * supers, LANES)
    hbm = pl.BlockSpec(memory_space=pl.ANY)
    off, res = pl.pallas_call(
        functools.partial(fused_kernel, n_r, n_c, supers, width, rows_dev, total_rows // pattern.shape[1], PARTS),
        out_shape=(
            pltpu.VMEM((rows_dev * supers * nb, LANES), jnp.float32),
            pltpu.VMEM((supers, 2, packed, LANES), jnp.float32),
        ),
        in_specs=[hbm, hbm, hbm, hbm],
        out_specs=(hbm, hbm),
        scratch_shapes=[
            pltpu.SMEM(pattern.shape, jnp.int32),
            f32(*sigma_anc.shape),
            f32(*linear.shape),
            f32(supers, rows_dev, width),
            f32(n_r * rows_dev, n_c * rows_dev),
            f32(2, n_c, rows_dev, width),
            f32(2, n_c, 2 * rows_dev, n_c * rows_dev),
            f32(width, width),
            f32(n_r, 2 * rows_dev, width),
            f32(2 * n_r * rows_dev, width),
            f32(2 * n_r * rows_dev, width),
            f32(slots, n_r, 2, rows_dev, LANES),
            f32(n_r, slots, rows_dev, LANES),
            f32(packed, LANES),
            f32(PARTS, q, LANES),
            f32(PARTS, q, LANES),
            f32(*linear.shape),
            f32(8 * packed + 8 * n_r * rows_dev * nb, LANES),
            dma(7 + n_c + 1),
            dma(3 * n_c), dma(n_c + 1), dma(n_r), dma(1), dma(1), dma(2), dma(PARTS),
            dma(2 * supers * PARTS), dma(1), dma(1), dma(4),
        ],
        compiler_params=pltpu.CompilerParams(
            collective_id=0, has_side_effects=True, vmem_limit_bytes=58 * 1024 * 1024
        ),
    )(sigma_anc, linear, diag_inverse, pattern)
    off, diag = pl.pallas_call(
        functools.partial(unpack_kernel, supers, nb),
        out_shape=(
            jax.ShapeDtypeStruct(off.shape, jnp.float32),
            jax.ShapeDtypeStruct((supers, width, width), jnp.float32),
        ),
        in_specs=[vm, vm],
        out_specs=(hbm, hbm),
        scratch_shapes=[f32(supers, width, width), dma(supers * nb + 1)],
        compiler_params=pltpu.CompilerParams(vmem_limit_bytes=8 * 1024 * 1024),
    )(off, res)
    off = jnp.transpose(off.reshape(rows_dev, nb, supers, LANES), (0, 2, 1, 3))
    return off.reshape(anc_factor.shape), diag


def fits(sigma_anc, anc_factor, diag_inverse):
    rows_dev, supers, width = anc_factor.shape
    n_r = lax.axis_size("row")
    n_c = lax.axis_size("col")
    nb = width // LANES
    return (
        n_r == n_c
        and n_r == 2 * supers
        and supers == 2
        and sigma_anc.shape[0] == sigma_anc.shape[1]
        and diag_inverse.shape[2] % LANES == 0
        and nb % 4 == 0
        and rows_dev % (2 * SUBLANES) == 0
        and width % (n_c * SUBLANES) == 0
        and len(pairs_of(nb)[0]) == len(pairs_of(nb)[1])
        and (len(pairs_of(nb)[0]) * LANES) % (2 * PARTS * SUBLANES) == 0
    )


def plain_body(sigma_anc, anc_factor, diag_inverse, pattern):
    precise = lax.Precision.HIGHEST
    rows_dev, supers, super_width = anc_factor.shape
    row_count = lax.axis_size("row")
    col_count = lax.axis_size("col")
    position = lax.axis_index("row") * col_count + lax.axis_index("col")
    total_rows = rows_dev * row_count * col_count
    block_size = total_rows // pattern.shape[1]
    flat_mask = jnp.repeat(pattern.astype(jnp.float32), block_size, axis=1)
    own_mask = jnp.transpose(lax.dynamic_slice_in_dim(flat_mask, position * rows_dev, rows_dev, 1))[
        :, :, None
    ]
    device_total = row_count * col_count
    share = -(-super_width // device_total)
    masked_factor = anc_factor * own_mask
    flattened = masked_factor.reshape(rows_dev, -1)
    gathered = lax.all_gather(flattened, "row", axis=0, tiled=True)
    stacked = gathered.reshape(row_count, rows_dev, flattened.shape[1])
    turned = lax.all_to_all(stacked, "col", split_axis=0, concat_axis=1, tiled=True)
    column_block = turned.reshape(row_count * rows_dev, flattened.shape[1])
    summed_rows = lax.psum_scatter(
        jnp.dot(sigma_anc, column_block, precision=precise, preferred_element_type=jnp.float32),
        "col",
        scatter_dimension=0,
        tiled=True,
    )
    off_factor = -(summed_rows.reshape(masked_factor.shape) * own_mask)
    both_rows = jnp.concatenate([masked_factor, off_factor], axis=0)
    column_piece = lax.all_gather(diag_inverse, "row", axis=2, tiled=True)
    product = jnp.einsum("rsk,skj->rsj", both_rows, column_piece, precision=precise)
    own_rows = lax.dynamic_slice_in_dim(column_piece, position * share, share, 1)
    scaled = product[:rows_dev]
    sel_off = product[rows_dev:]
    diag_term = jnp.einsum("skj,skl->sjl", own_rows, own_rows, precision=precise)
    partial_value = diag_term - jnp.einsum("rsj,rsl->sjl", scaled, sel_off, precision=precise)
    sel_diag = lax.psum(partial_value, ("row", "col"))
    return (sel_off, sel_diag)


def body(sigma_anc, anc_factor, diag_inverse, pattern):
    run = fused_body if fits(sigma_anc, anc_factor, diag_inverse) else plain_body
    return run(sigma_anc, anc_factor, diag_inverse, pattern)


def solution(mesh):
    return jax.shard_map(
        body,
        mesh=mesh,
        in_specs=(
            P(("grp", "row"), "col"),
            P(("grp", "row", "col"), None, None),
            P("grp", None, "row"),
            P(),
        ),
        out_specs=(P(("grp", "row", "col"), None, None), P("grp", None, None)),
        check_vma=False,
    )
```

```python
import functools
import math

import jax
import jax.numpy as jnp
from jax import lax
from jax.experimental import pallas as pl
from jax.experimental.pallas import tpu as pltpu
from jax.sharding import PartitionSpec as P

LANES = 128
SUBLANES = 8
PARTS = 4


def split(x):
    high = x.astype(jnp.bfloat16)
    low = (x - high.astype(jnp.float32)).astype(jnp.bfloat16)
    return high, low


def dot3(a, b, contract=((1,), (0,))):
    (ah, al), (bh, bl) = a, b
    f = lambda u, v: lax.dot_general(u, v, (contract, ((), ())), preferred_element_type=jnp.float32)
    return f(ah, bh) + (f(ah, bl) + f(al, bh))


def columns_of(nb):
    return [[j for j in range(nb) if (j + j // 2) % 2 == core] for core in range(2)]


def pairs_of(nb):
    columns = columns_of(nb)
    pairs = [[], []]
    every = [(i, j) for i in range(nb) for j in range(i + 1)]
    owners = lambda pair: [core for core in range(2) if pair[0] in columns[core] or pair[1] in columns[core]]
    for pair in sorted(every, key=lambda p: len(owners(p))):
        pairs[min(owners(pair), key=lambda core: len(pairs[core]))].append(pair)
    return pairs


def fused_kernel(
    n_r, n_c, supers, width, rows_dev, block_size, parts,
    sig_hbm, a_hbm, d_ref, pat_hbm,
    off_out, res,
    pat_ref, sig_ref, a_ref, av, sig_t, wz, sq, dfull, scl, vpart, vrecv, of, offr, gpart, grecv, mine, off_ref, spare,
    send_sems, s_w, s_sq, s_d, s_scl, s_v, s_off, s_h, s_g, s_sib, s_mine, local_sems,
):
    r = lax.axis_index("row")
    c = lax.axis_index("col")
    x = r // 2
    k = r % 2
    away = 1 - x
    sib = 2 * x + 1 - k
    par = 2 * away + k
    dia = 2 * away + 1 - k
    piece = width // n_r
    nb = width // LANES
    block_rows = rows_dev * n_c
    side_rows = 2 * rows_dev
    columns = columns_of(nb)
    pairs = pairs_of(nb)
    q = len(pairs[0]) * LANES // (2 * parts)
    low = n_c // 2 - 1
    side = c // 2
    mate = 4 * side + 1 - c
    hub = low + side
    is_hub = hub == c
    is_edge = hub != c
    single = [[] for _ in range(n_c)]
    bulk = [[0, 0] for _ in range(n_c)]
    late = [0]
    direct = parts // 2
    bulk_slot, v_slot, single_slot = 4, 6, 7

    def copy_to(src, dst, rsem, row, col, slot):
        return pltpu.make_async_remote_copy(
            src_ref=src, dst_ref=dst, send_sem=send_sems.at[slot], recv_sem=rsem,
            device_id={"row": row, "col": col}, device_id_type=pl.DeviceIdType.MESH,
        )

    def at_each_col(hub_part, edge_part=None):
        for cc in range(n_c):
            hub_col = low + cc // 2
            part = hub_part if cc == hub_col else edge_part
            if part is not None:
                pl.when(c == cc)(functools.partial(part, cc, n_c - 1 - cc))

    def post(cc, refs, row, col):
        bulk[cc][late[0]] += math.prod(refs()[0].shape)
        copy_to(*refs(), row, col, bulk_slot + late[0]).start()

    def post_hub(core, refs, row, col):
        if core == 0:
            for cc in (low, low + 1):
                bulk[cc][late[0]] += math.prod(refs()[0].shape)
        copy_to(*refs(), row, col, bulk_slot + late[0]).start()

    def off_refs(row, col, kind):
        return lambda: (of.at[:, row, col - 2 * side], offr.at[r], s_off.at[kind])

    def post_single(cc, refs, row, col):
        slot = single_slot + len(single[cc])
        make = lambda: copy_to(*refs(), row, col, slot)
        make().start()
        single[cc].append(make)

    def wait_sends(part):
        def at(cc, *_):
            whole = spare.at[pl.ds(0, bulk[cc][part] // LANES), :]
            pltpu.make_async_copy(whole, whole, send_sems.at[bulk_slot + part]).wait()
            if part == 0:
                for make in single[cc]:
                    make().wait_send()

        at_each_col(at, at)

    def wait_recv(dst, rsem):
        pltpu.make_async_copy(dst, dst, rsem).wait()

    loads = [
        pltpu.make_async_copy(a_hbm, a_ref, local_sems.at[2]),
        pltpu.make_async_copy(sig_hbm, sig_ref, local_sems.at[3]),
        pltpu.make_async_copy(pat_hbm, pat_ref, local_sems.at[1]),
    ]
    for cp in loads:
        cp.start()
    barrier = pltpu.get_barrier_semaphore()
    sig = lambda row, col: pl.semaphore_signal(
        barrier, inc=1, device_id={"row": row, "col": col}, device_id_type=pl.DeviceIdType.MESH
    )
    for dc in range(1, n_c):
        sig(r, (c + dc) % n_c)
    for row in (sib, par, dia):
        sig(row, c)
        sig(row, mate)

    def mask_of(first, rows, s):
        row = first + lax.broadcasted_iota(jnp.int32, (rows, 1), 0)
        m = jnp.zeros((rows, 1), jnp.float32)
        for b in range(pat_ref.shape[1]):
            inside = (row >= b * block_size) & (row < (b + 1) * block_size)
            m = jnp.where(inside, pat_ref[s, b].astype(jnp.float32), m)
        return m

    loads[2].wait()
    loads[0].wait()
    for s in range(supers):
        mask = mask_of((r * n_c + c) * rows_dev, rows_dev, s)
        for t in range(nb):
            rows = a_ref[pl.ds(t * supers + s, rows_dev, stride=nb * supers), :]
            av[s, :, t * LANES : (t + 1) * LANES] = rows * mask
    loads[1].wait()
    sig_t[...] = jnp.transpose(sig_ref[...])

    pl.semaphore_wait(barrier, n_c + 5)

    rows_w = lambda own, j: (wz.at[own, j], s_w.at[own * n_c + j])
    rows_s = lambda own, j: (sq.at[own, j], s_sq.at[n_c if own else j])
    half_rows = rows_dev // 2
    rows_h = lambda j, i: (wz.at[1, j, pl.ds(i * half_rows, half_rows), :], s_w.at[(1 + i) * n_c + j])
    half_of = lambda h: sig_t.at[pl.ds(h * side_rows, side_rows), :]
    d_slice = lambda rr: dfull.at[pl.ds(rr * piece, width - rr * piece), pl.ds(rr * piece, piece)]
    d_src = lambda rr, s: d_ref.at[s, pl.ds(rr * piece, width - rr * piece), :]
    sends_d = (is_hub & (k == 0)) | (is_edge & (k == 1))

    def hub_first(cc, other):
        post(cc, lambda: (av.at[away], *rows_w(1, cc)), par, c)
        post_single(cc, lambda: (half_of(1 - cc // 2), *rows_s(0, cc)), r, other)
        post(cc, lambda: (av.at[x], *rows_w(0, cc)), r, other)
        post_single(cc, lambda: (half_of(cc // 2), *rows_s(1, cc)), par, c)

    def edge_first(cc, other):
        near = low + cc // 2
        post(cc, lambda: (av.at[away], *rows_w(1, cc)), par, c)
        post(cc, lambda: (av.at[x], *rows_w(0, cc)), r, near)
        post_single(cc, lambda: (half_of(1 - cc // 2), *rows_s(0, cc)), r, n_c - 1 - near)

    at_each_col(hub_first, edge_first)
    for rr in range(n_r):
        @pl.when((r == rr) & sends_d)
        def _():
            copy_to(d_src(rr, away), d_slice(rr), s_d.at[rr], par, c, 0).start()

        @pl.when((r == rr) & is_hub)
        def _():
            copy_to(d_src(rr, x), d_slice(rr), s_d.at[rr], sib, c, 1).start()
            pltpu.make_async_copy(d_src(rr, x), d_slice(rr), local_sems.at[0]).start()

    @pl.when(is_hub)
    def _():
        wz[0, c] = av[x]
        sq[0, c] = sig_t[pl.ds(pl.multiple_of(side * side_rows, SUBLANES), side_rows), :]
        for rr in range(1, n_r):
            dfull[0 : rr * piece, rr * piece : (rr + 1) * piece] = jnp.zeros((rr * piece, piece), jnp.float32)

    def hub_pass(cc, other):
        edge = 0 if cc == low else n_c - 1
        wait_recv(*rows_w(1, cc))
        post(cc, lambda: (wz.at[1, cc], *rows_w(1, cc)), r, other)
        wait_recv(*rows_w(0, edge))
        post(cc, lambda: (wz.at[0, edge], *rows_w(0, edge)), r, other)
        for j in (other, n_c - 1 - edge):
            wait_recv(*rows_s(0, j))
            post_single(cc, lambda j=j: (sq.at[0, j], *rows_s(1, j)), par, c)

    def hub_pass_last(cc, other):
        edge = 0 if cc == low else n_c - 1
        for i in range(2):
            wait_recv(*rows_h(edge, i))
            post(cc, lambda i=i: (rows_h(edge, i)[0], *rows_h(edge, i)), r, other)
        wait_recv(*rows_s(0, edge))
        post_single(cc, lambda: (sq.at[0, edge], *rows_s(1, edge)), par, c)

    def edge_pass(cc, other):
        wait_recv(*rows_w(1, cc))
        for i in range(2):
            post(cc, lambda i=i: (rows_h(cc, i)[0], *rows_h(cc, i)), r, low + cc // 2)
        post_single(cc, lambda: (half_of(cc // 2), *rows_s(0, cc)), r, low + cc // 2)

    at_each_col(hub_pass, edge_pass)
    at_each_col(hub_pass_last)
    for rr in range(n_r):
        @pl.when((rr == par) & is_hub)
        def _():
            @pl.when(k == 0)
            def _():
                wait_recv(d_slice(rr), s_d.at[rr])
                copy_to(d_slice(rr), d_slice(rr), s_d.at[rr], sib, c, 2).start()

        @pl.when((rr == par) & is_edge & (k == 1))
        def _():
            wait_recv(d_slice(rr), s_d.at[rr])
            copy_to(d_slice(rr), d_slice(rr), s_d.at[rr], r, hub, 3).start()
    for rr in range(n_r):
        @pl.when((rr == par) & is_hub & (k == 1))
        def _():
            wait_recv(d_slice(rr), s_d.at[rr])
            copy_to(d_slice(rr), d_slice(rr), s_d.at[rr], sib, c, 2).start()
    def v_of(own):
        sigma = split(sq[own].reshape(n_r * side_rows, block_rows))
        return sigma, split(wz[own].reshape(block_rows, width))

    def hub_wait(own, cc, other):
        edge = 0 if cc == low else n_c - 1
        wait_recv(*rows_w(own, other))
        for i in range(2):
            if own == 1:
                wait_recv(*rows_h(n_c - 1 - edge, i))
            elif i == 0:
                wait_recv(*rows_w(0, n_c - 1 - edge))
        if own == 1:
            wait_recv(sq.at[1], s_sq.at[n_c])

    at_each_col(functools.partial(hub_wait, 0))

    @pl.when(is_hub)
    def _():
        vpart[...] = dot3(*v_of(0))

    for rr in range(n_r):
        @pl.when(((rr == sib) | (rr == dia)) & is_hub)
        def _():
            wait_recv(d_slice(rr), s_d.at[rr])

        @pl.when((rr == r) & is_hub)
        def _():
            pltpu.make_async_copy(d_src(rr, x), d_slice(rr), local_sems.at[0]).wait()

    rows_at = lambda h, i: pl.ds((h * parts + i) * q, q)
    over_rows = ((0,), (0,))
    lanes = lambda j: slice(j * LANES, (j + 1) * LANES)
    cut = lambda pair, j: (pair[0][:, lanes(j)], pair[1][:, lanes(j)])
    mask_rows = lambda: jnp.concatenate(
        [mask_of((rr * n_c + 2 * side) * rows_dev, side_rows, x) for rr in range(n_r)], axis=0
    )

    @pl.when(is_hub)
    def _():
        own = [wz[o, pl.ds(2 * side, 2)].reshape(side_rows, width) for o in range(2)]
        near = split(jnp.concatenate(own, axis=0))
        for j in range(0, width, LANES):
            ds = split(dfull[j:, j : j + LANES])
            v = dot3((near[0][:, j:], near[1][:, j:]), ds)
            scl[r, :, j : j + LANES] = v[:side_rows]
            scl[par, :, j : j + LANES] = v[side_rows:]

    def hub_scl(cc, *_):
        post(cc, lambda: (scl.at[r], scl.at[r], s_scl.at[0]), sib, c)
        post(cc, lambda: (scl.at[par], scl.at[par], s_scl.at[0]), sib, c)

    at_each_col(hub_scl)

    @pl.when(is_hub)
    def _():
        dz = split(dfull[pl.ds(pl.multiple_of(side * (width // 2), SUBLANES), width // 2), :])
        for core in range(2):
            @pl.when(k == core)
            def _():
                for b, (i, j) in enumerate(pairs[core]):
                    gpart[lanes(b), :] = dot3(cut(dz, i), cut(dz, j), over_rows)

    at_each_col(functools.partial(hub_wait, 1))
    far = n_c - 1 - c

    def sum_pairs(core, own_side, all_scl, ofs):
        first = (1 - own_side) * parts * q
        order = sorted(range(len(pairs[core])), key=lambda b: ((b + 1) * LANES <= first, b))
        left_parts = list(range(parts))
        ready = set()
        for b in order:
            i, j = pairs[core][b]
            left, right = (cut(all_scl, i), ofs[j]) if j in ofs else (ofs[i], cut(all_scl, j))
            gpart[lanes(b), :] += dot3(left, right, over_rows)
            ready.add(b)
            for part in list(left_parts):
                at = first + part * q
                if set(range(at // LANES, (at + q - 1) // LANES + 1)) <= ready:
                    left_parts.remove(part)
                    refs = lambda part=part: (gpart.at[rows_at(1 - own_side, part), :], grecv.at[part], s_h.at[part])
                    if core == 0:
                        bulk[low + own_side][0] += math.prod(refs()[0].shape)
                    copy_to(*refs(), r, far, bulk_slot).start()

    v_cols = lambda h: slice(h * (width // 2), (h + 1) * (width // 2))

    @pl.when(is_hub)
    def _():
        sigma, ws = v_of(1)
        for h in range(2):
            wide = (ws[0][:, v_cols(h)], ws[1][:, v_cols(h)])
            vpart[:, v_cols(h)] = vpart[:, v_cols(h)] + dot3(sigma, wide)
            copy_to(vpart.at[:, v_cols(h)], vrecv.at[:, v_cols(h)], s_v.at[0], sib, c, v_slot).start()

        wait_recv(scl.at[pl.ds(0, 2)], s_scl.at[0])
        all_scl = split(scl[...].reshape(n_r * side_rows, width))
        wait_recv(vrecv, s_v.at[0])
        vs = split((vpart[...] + vrecv[...]) * mask_rows())
        for core in range(2):
            @pl.when(k == core)
            def _():
                ofs = {}
                at = columns[core][0] * LANES
                d_cols = jnp.concatenate([dfull[at:, lanes(j)] for j in columns[core]], axis=1)
                v = dot3((vs[0][:, at:], vs[1][:, at:]), split(d_cols))
                for slot, j in enumerate(columns[core]):
                    part = v[:, lanes(slot)]
                    of[slot] = part.reshape(n_r, 2, rows_dev, LANES)
                    ofs[j] = split(part)
                for row, col, kind in ((par, c, 1), (dia, c, 1), (r, mate, 0), (sib, mate, 0), (sib, c, 0), (par, mate, 1), (dia, mate, 1)):
                    post_hub(core, off_refs(row, c if col is c else mate, kind), row, col)
                pltpu.make_async_copy(*off_refs(r, c, 0)()).start()
                for own_side in range(2):
                    pl.when(side == own_side)(functools.partial(sum_pairs, core, own_side, all_scl, ofs))

    chunk = lambda s, h, i: (res.at[s, k, rows_at(h, i), :], s_g.at[(s * 2 + h) * parts + i])
    held = lambda s, h, i: res.at[s, k, rows_at(h, i), :]

    late[0] = 1

    def forward(cc, s, h, i, row, col):
        post(cc, lambda: (held(s, h, i), *chunk(s, h, i)), row, col)

    def to_sib(cc, s, h, i):
        post(cc, lambda: (held(s, h, i), held(s, h, i), s_sib.at[0]), sib, c)

    def hub_reduce(cc, other):
        h = cc // 2
        edge = 0 if cc == low else n_c - 1
        for i in range(parts):
            wait_recv(grecv.at[i], s_h.at[i])
            mine[i] = gpart[rows_at(h, i), :] + grecv[i]
            pltpu.make_async_copy(mine.at[i], held(x, h, i), s_mine.at[0]).start()
            for row, col in ((par, c), (r, other), (r, edge)):
                post(cc, lambda i=i: (mine.at[i], *chunk(x, h, i)), row, col)
            post(cc, lambda i=i: (mine.at[i], held(x, h, i), s_sib.at[0]), sib, c)

    at_each_col(hub_reduce)

    def put_off(own):
        first = x if own else away
        wait_recv(offr.at[pl.ds(2 * first, 2)], s_off.at[0 if own else 1])
        for s in range(supers):
            @pl.when(first == s)
            def _():
                for row in (2 * s, 2 * s + 1):
                    for slot, t in enumerate(columns[row % 2]):
                        at = pl.ds(t * supers + s, rows_dev, stride=nb * supers)
                        off_ref[at, :] = -offr[row, slot]

    off_copy = lambda: pltpu.make_async_copy(off_ref, off_out, local_sems.at[2])
    put_off(True)

    @pl.when(is_hub)
    def _():
        put_off(False)
        off_copy().start()

    wait_sends(0)

    def hub_gather(cc, other):
        h = cc // 2
        edge = 0 if cc == low else n_c - 1
        for i in range(parts):
            wait_recv(*chunk(x, 1 - h, i))
            forward(cc, x, 1 - h, i, r, edge)
            forward(cc, x, 1 - h, i, par, c)
            wait_recv(*chunk(away, h, i))
            to_sib(cc, x, 1 - h, i)
            to_sib(cc, away, h, i)
        for i in range(direct, parts):
            forward(cc, away, h, i, r, n_c - 1 - edge)
        for i in range(parts):
            wait_recv(*chunk(away, 1 - h, i))
            to_sib(cc, away, 1 - h, i)

    def edge_gather(cc, *_):
        h = cc // 2
        for i in range(parts):
            wait_recv(*chunk(x, h, i))
            forward(cc, x, h, i, par, c)
            to_sib(cc, x, h, i)
        put_off(False)
        off_copy().start()
        for i in range(direct):
            wait_recv(*chunk(x, 1 - h, i))
            forward(cc, x, 1 - h, i, par, c)
            to_sib(cc, x, 1 - h, i)
        order = [(away, h, i) for i in range(parts)]
        for i in range(direct):
            order += [(away, 1 - h, i + direct), (away, 1 - h, i)]
        for i in range(direct, parts):
            order.insert(len(order) - (parts - 1 - i), (x, 1 - h, i))
        for s, g, i in order:
            wait_recv(*chunk(s, g, i))
            to_sib(cc, s, g, i)

    at_each_col(hub_gather, edge_gather)
    theirs = res.at[:, 1 - k]
    wait_recv(theirs, s_sib.at[0])
    @pl.when(is_hub)
    def _():
        pltpu.make_async_copy(mine, mine, s_mine.at[0]).wait()

    off_copy().wait()
    wait_sends(1)

    @pl.when(is_hub)
    def _():
        copy_to(vpart, vrecv, s_v.at[0], sib, c, v_slot).wait_send()

    for rr in range(n_r):
        @pl.when((r == rr) & sends_d)
        def _():
            copy_to(d_src(rr, away), d_slice(rr), s_d.at[rr], par, c, 0).wait_send()

        @pl.when((r == rr) & is_hub)
        def _():
            copy_to(d_src(rr, x), d_slice(rr), s_d.at[rr], sib, c, 1).wait_send()

        @pl.when((rr == par) & is_hub)
        def _():
            copy_to(d_slice(rr), d_slice(rr), s_d.at[rr], sib, c, 2).wait_send()

        @pl.when((rr == par) & is_edge & (k == 1))
        def _():
            copy_to(d_slice(rr), d_slice(rr), s_d.at[rr], r, hub, 3).wait_send()


def unpack_kernel(supers, nb, off_in, res, off_out, diag_out, stage, sems):
    copies = [pltpu.make_async_copy(off_in, off_out, sems.at[supers * nb])]
    copies[0].start()
    place = {pair: (core, b) for core, some in enumerate(pairs_of(nb)) for b, pair in enumerate(some)}
    for s in range(supers):
        for i in range(nb):
            for j in range(nb):
                core, b = place[max(i, j), min(i, j)]
                v = res[s, core, b * LANES : (b + 1) * LANES, :]
                stage[s, i * LANES : (i + 1) * LANES, j * LANES : (j + 1) * LANES] = v if i >= j else jnp.transpose(v)
            at = (s, pl.ds(i * LANES, LANES))
            copies.append(pltpu.make_async_copy(stage.at[at], diag_out.at[at], sems.at[s * nb + i]))
            copies[-1].start()
    for cp in copies:
        cp.wait()


def fused_body(sigma_anc, anc_factor, diag_inverse, pattern):
    rows_dev, supers, width = anc_factor.shape
    n_r = lax.axis_size("row")
    n_c = lax.axis_size("col")
    total_rows = rows_dev * n_r * n_c
    nb = width // LANES
    packed = len(pairs_of(nb)[0]) * LANES
    q = packed // (2 * PARTS)
    slots = len(columns_of(nb)[0])
    f32 = lambda *shape: pltpu.VMEM(shape, jnp.float32)
    dma = lambda n: pltpu.SemaphoreType.DMA((n,))
    vm = pl.BlockSpec(memory_space=pltpu.VMEM)
    linear = jnp.transpose(anc_factor.reshape(rows_dev, supers, nb, LANES), (0, 2, 1, 3))
    linear = linear.reshape(rows_dev * nb * supers, LANES)
    hbm = pl.BlockSpec(memory_space=pl.ANY)
    off, res = pl.pallas_call(
        functools.partial(fused_kernel, n_r, n_c, supers, width, rows_dev, total_rows // pattern.shape[1], PARTS),
        out_shape=(
            pltpu.VMEM((rows_dev * supers * nb, LANES), jnp.float32),
            pltpu.VMEM((supers, 2, packed, LANES), jnp.float32),
        ),
        in_specs=[hbm, hbm, hbm, hbm],
        out_specs=(hbm, hbm),
        scratch_shapes=[
            pltpu.SMEM(pattern.shape, jnp.int32),
            f32(*sigma_anc.shape),
            f32(*linear.shape),
            f32(supers, rows_dev, width),
            f32(n_r * rows_dev, n_c * rows_dev),
            f32(2, n_c, rows_dev, width),
            f32(2, n_c, 2 * rows_dev, n_c * rows_dev),
            f32(width, width),
            f32(n_r, 2 * rows_dev, width),
            f32(2 * n_r * rows_dev, width),
            f32(2 * n_r * rows_dev, width),
            f32(slots, n_r, 2, rows_dev, LANES),
            f32(n_r, slots, rows_dev, LANES),
            f32(packed, LANES),
            f32(PARTS, q, LANES),
            f32(PARTS, q, LANES),
            f32(*linear.shape),
            f32(8 * packed + 8 * n_r * rows_dev * nb, LANES),
            dma(7 + n_c + 1),
            dma(3 * n_c), dma(n_c + 1), dma(n_r), dma(1), dma(1), dma(2), dma(PARTS),
            dma(2 * supers * PARTS), dma(1), dma(1), dma(4),
        ],
        compiler_params=pltpu.CompilerParams(
            collective_id=0, has_side_effects=True, vmem_limit_bytes=58 * 1024 * 1024
        ),
    )(sigma_anc, linear, diag_inverse, pattern)
    off, diag = pl.pallas_call(
        functools.partial(unpack_kernel, supers, nb),
        out_shape=(
            jax.ShapeDtypeStruct(off.shape, jnp.float32),
            jax.ShapeDtypeStruct((supers, width, width), jnp.float32),
        ),
        in_specs=[vm, vm],
        out_specs=(hbm, hbm),
        scratch_shapes=[f32(supers, width, width), dma(supers * nb + 1)],
        compiler_params=pltpu.CompilerParams(vmem_limit_bytes=8 * 1024 * 1024),
    )(off, res)
    off = jnp.transpose(off.reshape(rows_dev, nb, supers, LANES), (0, 2, 1, 3))
    return off.reshape(anc_factor.shape), diag


def fits(sigma_anc, anc_factor, diag_inverse):
    rows_dev, supers, width = anc_factor.shape
    n_r = lax.axis_size("row")
    n_c = lax.axis_size("col")
    nb = width // LANES
    return (
        n_r == n_c
        and n_r == 2 * supers
        and supers == 2
        and sigma_anc.shape[0] == sigma_anc.shape[1]
        and diag_inverse.shape[2] % LANES == 0
        and nb % 4 == 0
        and rows_dev % (2 * SUBLANES) == 0
        and width % (n_c * SUBLANES) == 0
        and len(pairs_of(nb)[0]) == len(pairs_of(nb)[1])
        and (len(pairs_of(nb)[0]) * LANES) % (2 * PARTS * SUBLANES) == 0
    )


def plain_body(sigma_anc, anc_factor, diag_inverse, pattern):
    precise = lax.Precision.HIGHEST
    rows_dev, supers, super_width = anc_factor.shape
    row_count = lax.axis_size("row")
    col_count = lax.axis_size("col")
    position = lax.axis_index("row") * col_count + lax.axis_index("col")
    total_rows = rows_dev * row_count * col_count
    block_size = total_rows // pattern.shape[1]
    flat_mask = jnp.repeat(pattern.astype(jnp.float32), block_size, axis=1)
    own_mask = jnp.transpose(lax.dynamic_slice_in_dim(flat_mask, position * rows_dev, rows_dev, 1))[
        :, :, None
    ]
    device_total = row_count * col_count
    share = -(-super_width // device_total)
    masked_factor = anc_factor * own_mask
    flattened = masked_factor.reshape(rows_dev, -1)
    gathered = lax.all_gather(flattened, "row", axis=0, tiled=True)
    stacked = gathered.reshape(row_count, rows_dev, flattened.shape[1])
    turned = lax.all_to_all(stacked, "col", split_axis=0, concat_axis=1, tiled=True)
    column_block = turned.reshape(row_count * rows_dev, flattened.shape[1])
    summed_rows = lax.psum_scatter(
        jnp.dot(sigma_anc, column_block, precision=precise, preferred_element_type=jnp.float32),
        "col",
        scatter_dimension=0,
        tiled=True,
    )
    off_factor = -(summed_rows.reshape(masked_factor.shape) * own_mask)
    both_rows = jnp.concatenate([masked_factor, off_factor], axis=0)
    column_piece = lax.all_gather(diag_inverse, "row", axis=2, tiled=True)
    product = jnp.einsum("rsk,skj->rsj", both_rows, column_piece, precision=precise)
    own_rows = lax.dynamic_slice_in_dim(column_piece, position * share, share, 1)
    scaled = product[:rows_dev]
    sel_off = product[rows_dev:]
    diag_term = jnp.einsum("skj,skl->sjl", own_rows, own_rows, precision=precise)
    partial_value = diag_term - jnp.einsum("rsj,rsl->sjl", scaled, sel_off, precision=precise)
    sel_diag = lax.psum(partial_value, ("row", "col"))
    return (sel_off, sel_diag)


def body(sigma_anc, anc_factor, diag_inverse, pattern):
    run = fused_body if fits(sigma_anc, anc_factor, diag_inverse) else plain_body
    return run(sigma_anc, anc_factor, diag_inverse, pattern)


def solution(mesh):
    return jax.shard_map(
        body,
        mesh=mesh,
        in_specs=(
            P(("grp", "row"), "col"),
            P(("grp", "row", "col"), None, None),
            P("grp", None, "row"),
            P(),
        ),
        out_specs=(P(("grp", "row", "col"), None, None), P("grp", None, None)),
        check_vma=False,
    )
```
